32 devices in a mesh: seq: 8 (over z, y), fsdp: 4 (over x, core).
Axes of the slice: x: 2, y: 2, z: 4, core: 2. Of those that a mesh axis runs over, the one named last changes fastest.
Arguments:
- queries: bfloat16 [1024, 2048], P('seq', 'fsdp'), may hold values from -260 to 260
- layer_input: bfloat16 [1024, 4096], P('seq'), may hold values from -6 to 6
- w_key: bfloat16 [4096, 512], P('seq', 'fsdp'), may hold values from -0.09375 to 0.09375
- w_value: bfloat16 [4096, 512], P('seq', 'fsdp'), may hold values from -0.09375 to 0.09375
- grad_out: bfloat16 [1024, 2048], P('seq', 'fsdp'), may hold values from -6 to 6
Outputs:
- attn_out: bfloat16 [1024, 2048], P('seq', 'fsdp')
- grad_queries: bfloat16 [1024, 2048], P('seq', 'fsdp')
- grad_input: bfloat16 [1024, 4096], P('seq', 'fsdp')
- grad_w_key: float32 [4096, 512], P('seq', 'fsdp')
- grad_w_value: float32 [4096, 512], P('seq', 'fsdp')
The draws below stay inside these ranges and needn't reach their ends.
All inputs are finite; a program needn't handle non-finite values.
Results may differ from the reference program's by a relative error of at most 0.04.
Values may be sent and summed in bfloat16 or wider, within the bound.
A program may use at most 64 MiB of HBM per device.

```python
import math
import jax
import jax.numpy as jnp
from jax import lax

D = 4096
HD = 128
KV_HEADS = 4
GROUP = 4
QW = 2048
KVW = 512
TOKENS = 1024


def draw_queries(key, part):
    base = jnp.clip(jax.random.normal(key, (TOKENS, QW), jnp.float32), -6.0, 6.0)
    return base.astype(jnp.bfloat16)


def level_of(rng, dims, pieces, smallest, top_value):
    factor_of = 1.0
    for axis_at, shards_of in pieces:
        heights = jax.random.uniform(jax.random.fold_in(jax.random.fold_in(rng, 6), axis_at), (shards_of,), jnp.float32, smallest / len(pieces), top_value / len(pieces))
        factor_of = factor_of * jnp.repeat(jnp.exp(heights), dims[axis_at] // shards_of).reshape((-1,) + (1,) * (len(dims) - 1 - axis_at))
    return factor_of


def scatter_about(own_key, shape, deviation, limit, pieces=(), kind=jnp.bfloat16):
    result = jax.random.normal(own_key, shape, jnp.float32) * deviation
    if len(pieces) > 0:
        result = level_of(own_key, shape, pieces, -0.22, 0.18) * result
    return jnp.clip(result, min=-limit, max=limit).astype(kind)


def setup_inputs(seed: int = 0) -> dict:
    arg_keys = jax.random.split(jax.random.key(seed), 6)
    return {
        "queries": draw_queries(jax.random.fold_in(arg_keys[5], 71), 0),
        "layer_input": scatter_about(arg_keys[1], (TOKENS, D), 1.0, 6.0, ((0, 8),)),
        "w_key": scatter_about(arg_keys[2], (D, KVW), D ** -0.5, 0.09375, ((0, 8), (1, 4))),
        "w_value": scatter_about(arg_keys[3], (D, KVW), D ** -0.5, 0.09375, ((0, 8), (1, 4))),
        "grad_out": scatter_about(arg_keys[4], (TOKENS, QW), 1.0, 6.0, ((0, 8), (1, 4))),
    }


ROPE_BASE = 500000.0
NEG = -1.0e30


def rope_tables(positions, half):
    freq = ROPE_BASE ** (-(jnp.arange(half, dtype=jnp.float32) * (2.0 / (2 * half))))
    angle = positions.astype(jnp.float32)[:, None] * freq[None, :]
    return jnp.cos(angle), jnp.sin(angle)


def rotate(heads, cosine, sine):
    half = heads.shape[-1] // 2
    first = heads[..., :half]
    second = heads[..., half:]
    cos_b = cosine[:, None, :]
    sin_b = sine[:, None, :]
    return jnp.concatenate([first * cos_b - second * sin_b, second * cos_b + first * sin_b], axis=-1)


def to_low(array):
    return lax.optimization_barrier(array.astype(jnp.bfloat16)).astype(jnp.float32)


def reference(queries, layer_input, w_key, w_value, grad_out):
    scale = HD ** -0.5
    key_linear = jnp.dot(layer_input, w_key, preferred_element_type=jnp.float32).reshape(TOKENS, KV_HEADS, HD)
    value_rows = jnp.dot(layer_input, w_value, preferred_element_type=jnp.float32).astype(jnp.bfloat16)
    value_rows = value_rows.reshape(TOKENS, KV_HEADS, HD)
    positions = jnp.arange(TOKENS, dtype=jnp.int32)
    cosine, sine = rope_tables(positions, HD // 2)
    keys = rotate(key_linear, cosine, sine).astype(jnp.bfloat16)
    keys_wide = keys.astype(jnp.float32)
    values_wide = value_rows.astype(jnp.float32)
    query = queries.astype(jnp.float32).reshape(TOKENS, KV_HEADS, GROUP, HD)
    upstream = grad_out.astype(jnp.float32).reshape(TOKENS, KV_HEADS, GROUP, HD)
    block = math.gcd(TOKENS, 256)
    count = TOKENS // block
    key_pos = jnp.arange(TOKENS, dtype=jnp.int32)

    def block_scores(index):
        start = (index * block).astype(jnp.int32)
        rows = lax.dynamic_slice_in_dim(query, start, block, 0)
        scores = jnp.einsum("qhgd,khd->hgqk", rows, keys_wide) * scale
        query_pos = start + jnp.arange(block, dtype=jnp.int32)
        mask = key_pos[None, :] <= query_pos[:, None]
        return rows, jnp.where(mask, scores, NEG), mask

    def forward_block(index):
        rows, scores, mask = block_scores(index)
        top = jnp.max(scores, axis=-1, keepdims=True)
        total = jnp.sum(jnp.where(mask, jnp.exp(scores - top), 0.0), axis=-1, keepdims=True)
        lse = top + jnp.log(total)
        probs = to_low(jnp.where(mask, jnp.exp(scores - lse), 0.0))
        return jnp.einsum("hgqk,khd->qhgd", probs, values_wide), lse[..., 0]

    outs, lses = lax.map(forward_block, jnp.arange(count, dtype=jnp.int32))
    output = outs.reshape(TOKENS, KV_HEADS, GROUP, HD)
    lse_all = jnp.transpose(lses, (1, 2, 0, 3)).reshape(KV_HEADS, GROUP, TOKENS)
    delta_all = jnp.transpose(jnp.sum(upstream * output, axis=-1), (1, 2, 0))

    def backward_block(carry, index):
        key_acc, value_acc = carry
        rows, scores, mask = block_scores(index)
        start = (index * block).astype(jnp.int32)
        lse_blk = lax.dynamic_slice_in_dim(lse_all, start, block, 2)
        delta_blk = lax.dynamic_slice_in_dim(delta_all, start, block, 2)
        up_rows = lax.dynamic_slice_in_dim(upstream, start, block, 0)
        probs = jnp.where(mask, jnp.exp(scores - lse_blk[..., None]), 0.0)
        dprobs = jnp.einsum("qhgd,khd->hgqk", up_rows, values_wide)
        dscores = probs * (dprobs - delta_blk[..., None])
        value_acc = value_acc + jnp.einsum("hgqk,qhgd->khd", to_low(probs), up_rows)
        ds_low = to_low(dscores)
        query_grad = jnp.einsum("hgqk,khd->qhgd", ds_low, keys_wide) * scale
        key_acc = key_acc + jnp.einsum("hgqk,qhgd->khd", ds_low, rows) * scale
        return (key_acc, value_acc), query_grad.astype(jnp.bfloat16)

    zeros = jnp.zeros((TOKENS, KV_HEADS, HD), jnp.float32)
    (key_acc, value_acc), query_grads = lax.scan(backward_block, (zeros, zeros), jnp.arange(count, dtype=jnp.int32))
    key_grad = rotate(key_acc, cosine, -sine).astype(jnp.bfloat16).reshape(TOKENS, KVW)
    value_grad = value_acc.astype(jnp.bfloat16).reshape(TOKENS, KVW)
    grad_w_key = jnp.dot(layer_input.T, key_grad, preferred_element_type=jnp.float32)
    grad_w_value = jnp.dot(layer_input.T, value_grad, preferred_element_type=jnp.float32)
    grad_input = (jnp.dot(key_grad, w_key.T, preferred_element_type=jnp.float32)
                  + jnp.dot(value_grad, w_value.T, preferred_element_type=jnp.float32)).astype(jnp.bfloat16)
    attn_out = output.reshape(TOKENS, QW).astype(jnp.bfloat16)
    return attn_out, query_grads.reshape(TOKENS, QW), grad_input, grad_w_key, grad_w_value
```

```python
import functools
import math

import jax
import jax.numpy as jnp
import numpy as np
from jax import lax
from jax.experimental import pallas as pl
from jax.experimental.pallas import tpu as pltpu
from jax.sharding import PartitionSpec as P

HD = 128
ROPE_BASE = 500000.0
NEG = -1e30
MESH = pl.DeviceIdType.MESH
F32 = jnp.float32
BF16 = jnp.bfloat16


def loop(low, high, step):
    def run(i, carry):
        step(i)
        return carry

    lax.fori_loop(low, high, run, 0)


def dot_nn(a, b):
    return lax.dot_general(a, b, (((1,), (0,)), ((), ())), preferred_element_type=F32)


def dot_nt(a, b):
    return lax.dot_general(a, b, (((1,), (1,)), ((), ())), preferred_element_type=F32)


def dot_tn(a, b):
    return lax.dot_general(a, b, (((0,), (0,)), ((), ())), preferred_element_type=F32)


def block_of(ref, b, size):
    return ref.at[pl.ds(pl.multiple_of(b * size, size), size)]


def chunks_of(rows, inner):
    late = rows * 3 // 16 // 16 * 16 if inner == 2 else 0
    rest = rows - late
    pieces = 2 if rest >= 256 else 1
    size = rest // pieces // 16 * 16
    out, at = [], 0
    for i in range(pieces):
        count = size if i < pieces - 1 else rest - at
        out.append((at, count, False))
        at += count
    if late:
        out.append((at, late, True))
    return out


def kernel(cfg, *refs):
    n, nf, exchange = cfg
    q_hbm, x_hbm, wk_ref, wv_ref, g_hbm, freq_ref = refs[:6]
    refs = refs[6:]
    if not exchange:
        xt_in = refs[0]
        refs = refs[1:]
    ao_ref, gq_ref, gi_ref, gwk_ref, gwv_ref = refs[:5]
    (wk_all, wv_all, k_all, v_all, dk_all, dv_all, x_all, q_st, g_st, g_tr,
     s_scr, p_scr, ds_scr, m_scr, l_scr, o_acc, dq_acc, dkp, dvp,
     rk_send, rk_recv, rv_send, rv_recv, own_dk, own_dv, cos_scr, sin_scr,
     gi_send, gi_recv, gi_own,
     wk_s, wk_r, wv_s, wv_r, k_s, k_r, v_s, v_r, dk_s, dk_r, dv_s, dv_r,
     x_s, x_r, xf_s, xf_r, rk_s, rk_r, rv_s, rv_r, gi_s, gi_r,
     q_ref, x_ref, g_ref, in_s) = refs[5:]
    tok = x_ref.shape[0]
    rows, cols = wk_ref.shape
    group = q_ref.shape[1] // cols
    m_cols = group * tok
    part = rows // nf
    width = gi_ref.shape[1]
    total = n * tok
    span = ds_scr.shape[0]
    spans = total // span
    per_span = span // tok
    chunk = math.gcd(span, 256)
    scale = HD ** (-0.5)
    s = lax.axis_index("seq")
    f = lax.axis_index("fsdp")
    inner = 2 if n % 2 == 0 else 1
    outer = n // inner
    z = s // inner
    y = s % inner
    mate = z * inner + (inner - 1 - y)

    def copy(src, dst, send, recv, dev):
        return pltpu.make_async_remote_copy(
            src_ref=src, dst_ref=dst, send_sem=send, recv_sem=recv, device_id=dev,
            device_id_type=MESH,
        )

    barrier = pltpu.get_barrier_semaphore()

    def greet_seq(d):
        pl.semaphore_signal(
            barrier, inc=1, device_id=((s + d) % n, f), device_id_type=MESH)

    def greet_fsdp(d):
        pl.semaphore_signal(
            barrier, inc=1, device_id=(s, (f + d) % nf), device_id_type=MESH)

    loop(1, n, greet_seq)
    loop(1, nf, greet_fsdp)
    loads = [
        pltpu.make_async_copy(src, dst, in_s.at[i])
        for i, (src, dst) in enumerate((
            (wk_ref, block_of(wk_all, s, rows)), (wv_ref, block_of(wv_all, s, rows)),
            (x_hbm, x_ref), (q_hbm, q_ref), (g_hbm, g_ref)))
    ]
    for load in loads:
        load.start()

    def clear(b):
        at = pl.ds(pl.multiple_of(b * tok, tok), tok)
        k_all[at, :] = jnp.zeros((tok, cols), BF16)
        v_all[at, :] = jnp.zeros((tok, cols), BF16)

    loop(inner * (z + 1), n, clear)
    pl.semaphore_wait(barrier, n + nf - 2)

    class Gather:
        def __init__(self, ref, send, recv, causal=False):
            self.slot = lambda b: block_of(ref, b, tok)
            self.send, self.recv = send, recv
            self.give_to = outer - z if causal else outer
            self.take_from = z + 1 if causal else outer

        def outgoing(self, d):
            return copy(self.slot(s), self.slot(s), self.send.at[d], self.recv.at[s],
                        ((z + d) % outer * inner + y, f))

        def to_mate(self):
            return copy(self.slot(s), self.slot(s), self.send.at[0], self.recv.at[s], (mate, f))

        def arrived(self, b):
            copy(self.slot(b), self.slot(b), self.send.at[0], self.recv.at[b],
                 (mate, f)).wait_recv()

        def pass_on(self, d):
            b = (z - d + outer) % outer * inner + y
            return copy(self.slot(b), self.slot(b), self.send.at[outer + d], self.recv.at[b],
                        (mate, f))

        def start(self):
            if inner == 2:
                self.to_mate().start()
            loop(1, self.give_to, lambda d: self.outgoing(d).start())

        def forward(self):
            def step(d):
                self.arrived((z - d + outer) % outer * inner + y)
                if inner == 2:
                    self.pass_on(d).start()

            loop(1, self.take_from, step)

        def finish(self):
            if inner == 2:
                loop(0, self.take_from, lambda d: self.arrived(
                    (z - d + outer) % outer * inner + (inner - 1 - y)))

        def drain(self):
            if inner == 2:
                self.to_mate().wait_send()
            loop(1, self.give_to, lambda d: self.outgoing(d).wait_send())
            if inner == 2:
                loop(1, self.take_from, lambda d: self.pass_on(d).wait_send())

    pieces = chunks_of(rows, inner)

    class Weights:
        def __init__(self, ref, send, recv):
            self.ref, self.send, self.recv = ref, send, recv

        def hop(self, q, b, way):
            at, count, _ = pieces[q]
            ref = self.ref.at[pl.ds(pl.multiple_of(b * rows + at, 16), count)]
            dev = ((z + 1) * inner + y, (z - 1) * inner + y, mate)[way]
            return copy(ref, ref, self.send.at[q, way * n + b], self.recv.at[q, b], (dev, f))

        def arrived(self, q, b):
            self.hop(q, b, 2).wait_recv()

        def order(self, way):
            qs = list(range(len(pieces)))
            return qs[::-1] if way == 2 else qs

        def own(self, way, act):
            def go():
                for q in self.order(way):
                    getattr(self.hop(q, s, way), act)()

            if way == 0:
                pl.when(z < outer - 1)(go)
            elif way == 1:
                pl.when(z > 0)(go)
            elif inner == 2:
                go()

        def mates(self, act):
            for q, (_, _, late) in enumerate(pieces):
                if late:
                    if act == "start":
                        self.arrived(q, mate)
                    pl.when(z < outer - 1)(lambda q=q: getattr(self.hop(q, mate, 0), act)())
                    pl.when(z > 0)(lambda q=q: getattr(self.hop(q, mate, 1), act)())

        def relay(self, d, way, act):
            level = z - d if way == 0 else z + d
            more = z < outer - 1 if way == 0 else z > 0
            for q, (_, _, late) in enumerate(pieces):
                for line in range(inner) if late else (y,):
                    b = level * inner + line
                    if act == "start":
                        self.arrived(q, b)
                    pl.when(more)(lambda q=q, b=b: getattr(self.hop(q, b, way), act)())
                    if inner == 2 and not late:
                        getattr(self.hop(q, b, 2), act)()

        def relays(self, act, after=None):
            if after is not None:
                pl.when(z == 0)(lambda: after(0))
                pl.when(z == outer - 1)(lambda: after(1))
            self.mates(act)

            def step(d):
                @pl.when(z >= d)
                def _():
                    self.relay(d, 0, act)
                    if after is not None:
                        pl.when(z == d)(lambda: after(0))

                @pl.when(z + d < outer)
                def _():
                    self.relay(d, 1, act)
                    if after is not None:
                        pl.when(z + d == outer - 1)(lambda: after(1))

            loop(1, outer, step)
            if after is not None:
                after(2)

        def finish(self):
            if inner == 2:
                def step(level):
                    for q, (_, _, late) in enumerate(pieces):
                        if not late:
                            self.arrived(q, level * inner + (inner - 1 - y))

                loop(0, outer, step)

        def drain(self):
            for way in range(3):
                self.own(way, "wait_send")
            self.relays("wait_send")

    wk_gather = Weights(wk_all, wk_s, wk_r)
    wv_gather = Weights(wv_all, wv_s, wv_r)
    k_gather = Gather(k_all, k_s, k_r, causal=True)
    v_gather = Gather(v_all, v_s, v_r, causal=True)
    dk_gather = Gather(dk_all, dk_s, dk_r)
    dv_gather = Gather(dv_all, dv_s, dv_r)

    loads[0].wait()
    for way in (0, 1, 2):
        wk_gather.own(way, "start")
    for load in loads[1:]:
        load.wait()

    own_rows = pl.ds(pl.multiple_of(s * tok, tok), tok)
    if exchange:
        own_part = pl.ds(pl.multiple_of(f * part, 128), part)

        def x_src(b):
            return x_ref.at[:, pl.ds(pl.multiple_of(b * rows + f * part, 128), part)]

        def x_slot(b, at):
            return x_all.at[pl.ds(pl.multiple_of(b * tok, tok), tok), at]

        def x_copy(b):
            return copy(x_src(b), x_slot(s, own_part), x_s.at[b], x_r.at[s], (b, f))

        def x_arrived(b):
            copy(x_src(b), x_slot(b, own_part), x_s.at[b], x_r.at[b], (b, f)).wait_recv()

        def xf_copy(d):
            ref = x_all.at[:, own_part]
            return copy(ref, ref, xf_s.at[d], xf_r.at[f], (s, (f + d) % nf))

        def xf_arrived(d):
            b = (f + d) % nf
            ref = x_all.at[:, pl.ds(pl.multiple_of(b * part, 128), part)]
            copy(ref, ref, xf_s.at[d], xf_r.at[b], (s, b)).wait_recv()

        x_all[own_rows, own_part] = x_ref[
            :, pl.ds(pl.multiple_of(s * rows + f * part, 128), part)]

    for g in range(group):
        at = slice(g * tok, (g + 1) * tok)
        q_st[at, :] = q_ref[:, g * HD:(g + 1) * HD]
        up = g_ref[:, g * HD:(g + 1) * HD]
        g_st[at, :] = up
        g_tr[:, at] = up.astype(F32).T
    lane = lax.broadcasted_iota(jnp.int32, (tok, HD), 1)
    position = (s * tok + lax.broadcasted_iota(jnp.int32, (tok, HD), 0)).astype(F32)
    angle = position * freq_ref[...]
    cos_scr[...] = jnp.cos(angle)
    sin_scr[...] = jnp.where(lane < HD // 2, -jnp.sin(angle), jnp.sin(angle))

    wk_gather.relays("start", lambda way: wv_gather.own(way, "start"))
    wk_gather.finish()

    lin = dot_nn(x_ref[...], wk_all[...])
    turned = lin * cos_scr[...] + pltpu.roll(lin, HD // 2, 1) * sin_scr[...]
    k_all[own_rows, :] = turned.astype(BF16)
    k_gather.start()

    wv_gather.relays("start")
    k_gather.forward()
    wv_gather.finish()
    v_all[own_rows, :] = dot_nn(x_ref[...], wv_all[...]).astype(BF16)
    v_gather.start()
    if exchange:
        loop(0, s, lambda b: x_copy(b).start())
    k_gather.finish()

    def each_span(step):
        if spans == 1:
            step(0)
        else:
            loop(0, s * tok // span + 1, lambda i: step(pl.multiple_of(i * span, span)))

    def at_chunk(base, c):
        return pl.ds(base + c * chunk, chunk)

    def fold(value):
        return value.reshape(chunk // 8, 8, m_cols)

    column = jnp.concatenate(
        [lax.broadcasted_iota(jnp.int32, (chunk, tok), 1)] * group, axis=1)
    ahead = lax.broadcasted_iota(jnp.int32, (chunk, m_cols), 0) - column

    m_scr[...] = jnp.full(m_scr.shape, NEG, F32)
    l_scr[...] = jnp.zeros(l_scr.shape, F32)
    o_acc[...] = jnp.zeros(o_acc.shape, F32)
    dq_acc[...] = jnp.zeros(dq_acc.shape, F32)

    def score(base):
        for c in range(span // chunk):
            sc = dot_nt(k_all[at_chunk(base, c), :], q_st[...])
            sc = jnp.where(ahead <= s * tok - base - c * chunk, sc, NEG)
            s_scr[at_chunk(base, c), :] = sc
            m_scr[...] = jnp.maximum(m_scr[...], jnp.max(fold(sc), axis=0))

    each_span(score)
    top = jnp.max(m_scr[...], axis=0, keepdims=True)

    def weigh(base):
        for c in range(span // chunk):
            e = jnp.exp2((s_scr[at_chunk(base, c), :] - top) * (scale * math.log2(math.e)))
            s_scr[at_chunk(base, c), :] = e
            l_scr[...] += jnp.sum(fold(e), axis=0)

    each_span(weigh)
    inverse = 1.0 / jnp.sum(l_scr[...], axis=0, keepdims=True)

    def rs_copy(send, recv, send_sem, recv_sem, j):
        return copy(send.at[j], recv.at[s], send_sem.at[j], recv_sem.at[s], (j, f))

    def rk_copy(j):
        return rs_copy(rk_send, rk_recv, rk_s, rk_r, j)

    def rv_copy(j):
        return rs_copy(rv_send, rv_recv, rv_s, rv_r, j)

    def hand_out(base, low, high, partial, own, start):
        first = base // tok
        loop(first + low, jnp.minimum(first + high, s), start)
        if spans == 1:
            if high == per_span:
                own[...] = partial[own_rows, :]
        else:
            @pl.when(jnp.logical_and(s >= first + low, s < first + high))
            def _():
                own[...] = partial[pl.ds(pl.multiple_of(s * tok - base, tok), tok), :]

    def store_parts(base, c, value, partial, send):
        partial[c * chunk:(c + 1) * chunk, :] = value
        for i in range(chunk // tok):
            send[base // tok + c * (chunk // tok) + i] = value[i * tok:(i + 1) * tok].astype(BF16)

    def value_part(base):
        for c in range(span // chunk):
            p = s_scr[at_chunk(base, c), :] * inverse
            s_scr[at_chunk(base, c), :] = p
            low = p.astype(BF16)
            p_scr[at_chunk(base, c), :] = low
            store_parts(base, c, dot_nn(low, g_st[...]), dvp, rv_send)
        hand_out(base, 0, per_span, dvp, own_dv, lambda j: rv_copy(j).start())

    each_span(value_part)
    v_gather.forward()
    if exchange:
        loop(s + 1, n, lambda b: x_copy(b).start())
    v_gather.finish()

    def weighted(base):
        o_acc[...] += dot_tn(v_all[pl.ds(base, span), :], p_scr[pl.ds(base, span), :])

    each_span(weighted)
    delta = jnp.sum(g_tr[...] * o_acc[...], axis=0, keepdims=True)

    def key_part(base):
        halves = 2 if (span // chunk) % 2 == 0 else 1
        count = span // chunk // halves
        for half in range(halves):
            for c in range(half * count, (half + 1) * count):
                dp = dot_nt(v_all[at_chunk(base, c), :], g_st[...])
                ds = (s_scr[at_chunk(base, c), :] * (dp - delta)).astype(BF16)
                ds_scr[c * chunk:(c + 1) * chunk, :] = ds
                store_parts(base, c, dot_nn(ds, q_st[...]), dkp, rk_send)
            hand_out(base, half * per_span // halves, (half + 1) * per_span // halves, dkp, own_dk,
                     lambda j: rk_copy(j).start())
        dq_acc[...] += dot_tn(k_all[pl.ds(base, span), :], ds_scr[...])

    each_span(key_part)
    for g in range(group):
        at = slice(g * tok, (g + 1) * tok)
        ao_ref[:, g * HD:(g + 1) * HD] = o_acc[:, at].T.astype(BF16)
        gq_ref[:, g * HD:(g + 1) * HD] = (dq_acc[:, at] * scale).T.astype(BF16)

    if exchange:
        loop(0, s, x_arrived)
        loop(s + 1, n, x_arrived)
        loop(1, nf, lambda d: xf_copy(d).start())

    def take(recv, make, own):
        def step(j):
            make(j).wait_recv()
            own[...] += recv[j].astype(F32)

        loop(s + 1, n, step)

    def rv_from(j):
        return copy(rv_send.at[0], rv_recv.at[j], rv_s.at[0], rv_r.at[j], (mate, f))

    def rk_from(j):
        return copy(rk_send.at[0], rk_recv.at[j], rk_s.at[0], rk_r.at[j], (mate, f))

    take(rv_recv, rv_from, own_dv)
    dv_all[own_rows, :] = own_dv[...].astype(BF16)
    dv_gather.start()
    take(rk_recv, rk_from, own_dk)
    lin = own_dk[...] * scale
    turned = lin * cos_scr[...] - pltpu.roll(lin, HD // 2, 1) * sin_scr[...]
    dk_all[own_rows, :] = turned.astype(BF16)
    dk_gather.start()

    def input_term(b):
        at = pl.ds(pl.multiple_of(b * width, width), width)
        return (dot_nt(dk_all[own_rows, :], wk_all[at, :])
                + dot_nt(dv_all[own_rows, :], wv_all[at, :]))

    cores = 2 if nf % 2 == 0 else 1
    chips = nf // cores
    chip = f // cores
    core = f % cores
    twin = chip * cores + (cores - 1 - core)

    def gi_twin(o):
        return copy(gi_send.at[o], gi_recv.at[o], gi_s.at[o], gi_r.at[o], (s, twin))

    def gi_far(d):
        return copy(gi_send.at[chips + d], gi_recv.at[chips + chip], gi_s.at[chips + d],
                    gi_r.at[chips + chip], (s, (chip + d) % chips * cores + core))

    def twin_term(d):
        o = (chip + d) % chips
        gi_send[o] = input_term(o * cores + 1 - core).astype(BF16)
        gi_twin(o).start()

    def own_term(d):
        o = (chip + d) % chips
        gi_own[o] = input_term(o * cores + core)

    def join(d):
        o = (chip + d) % chips
        gi_twin(o).wait_recv()
        gi_own[o] += gi_recv[o].astype(F32)

    def far_term(d):
        if cores == 2:
            join(d)
        gi_send[chips + d] = gi_own[(chip + d) % chips].astype(BF16)
        gi_far(d).start()

    if cores == 2:
        loop(1, chips + 1, twin_term)
    loop(1, chips + 1, own_term)
    loop(1, chips, far_term)
    if cores == 2:
        join(0)

    def weight_grad(grads, out):
        if exchange:
            out[...] = dot_tn(grads[...], x_all[...]).T
        else:
            grad = None
            step = min(total, 1024)
            for at in range(0, total, step):
                term = dot_tn(xt_in[at:at + step, :], grads[at:at + step, :])
                grad = term if grad is None else grad + term
            out[...] = grad

    dv_gather.forward()
    dk_gather.forward()
    dv_gather.finish()
    if exchange:
        loop(1, nf, xf_arrived)
    weight_grad(dv_all, gwv_ref)
    dk_gather.finish()
    weight_grad(dk_all, gwk_ref)

    def gi_take(d):
        b = (chip + d) % chips
        copy(gi_send.at[chips + d], gi_recv.at[chips + b], gi_s.at[chips + d],
             gi_r.at[chips + b], (s, b * cores + core)).wait_recv()
        gi_own[chip] += gi_recv[chips + b].astype(F32)

    loop(1, chips, gi_take)
    gi_ref[...] = gi_own[chip].astype(BF16)

    for gather in (wk_gather, wv_gather, k_gather, v_gather, dk_gather, dv_gather):
        gather.drain()
    if exchange:
        loop(0, s, lambda b: x_copy(b).wait_send())
        loop(s + 1, n, lambda b: x_copy(b).wait_send())
        loop(1, nf, lambda d: xf_copy(d).wait_send())
    loop(0, s, lambda j: rv_copy(j).wait_send())
    loop(0, s, lambda j: rk_copy(j).wait_send())
    if cores == 2:
        loop(0, chips, lambda o: gi_twin(o).wait_send())
    loop(1, chips, lambda d: gi_far(d).wait_send())


def publish(*refs):
    count = len(refs) // 2
    sems = refs[-1]
    moves = [pltpu.make_async_copy(refs[i], refs[count + i], sems.at[i]) for i in range(count)]
    for move in moves:
        move.start()
    for move in moves:
        move.wait()


def body(n, nf, queries, layer_input, w_key, w_value, grad_out):
    tok, depth = layer_input.shape
    rows, cols = w_key.shape
    assert cols == HD
    group = queries.shape[1] // cols
    m_cols = group * tok
    part = rows // nf
    exchange = part % 128 == 0
    half = HD // 2
    freq = np.float32(ROPE_BASE) ** (-(np.arange(half, dtype=np.float32) * np.float32(2.0 / HD)))
    freq = jnp.asarray(np.concatenate([freq, freq])[None, :], F32)
    operands = [queries, layer_input, w_key, w_value, grad_out, freq]
    if not exchange:
        operands.append(
            lax.all_to_all(layer_input, "seq", split_axis=1, concat_axis=0, tiled=True))
    width = depth // nf
    total = n * tok
    span = math.gcd(total, 1024)
    pieces = len(chunks_of(rows, 2 if n % 2 == 0 else 1))
    vmem = pltpu.VMEM
    dma = pltpu.SemaphoreType.DMA
    scratch = [vmem((depth, cols), BF16)] * 2
    scratch += [vmem((total, cols), BF16)] * 4
    scratch += [
        vmem((total, rows) if exchange else (16, 128), BF16),
        vmem((m_cols, HD), BF16), vmem((m_cols, HD), BF16), vmem((HD, m_cols), F32),
        vmem((total, m_cols), F32), vmem((total, m_cols), BF16), vmem((span, m_cols), BF16),
        vmem((8, m_cols), F32), vmem((8, m_cols), F32),
        vmem((HD, m_cols), F32), vmem((HD, m_cols), F32),
        vmem((span, cols), F32), vmem((span, cols), F32),
    ]
    scratch += [vmem((n, tok, cols), BF16)] * 4
    scratch += [vmem((tok, cols), F32)] * 4
    scratch += [
        vmem((2 * nf, tok, width), BF16), vmem((2 * nf, tok, width), BF16),
        vmem((nf, tok, width), F32),
    ]
    scratch += [dma((pieces, 3 * n)), dma((pieces, n))] * 2
    scratch += [dma((n,)), dma((n,))] * 4
    scratch += [dma((n,)), dma((n,)), dma((nf,)), dma((nf,))]
    scratch += [dma((n,)), dma((n,))] * 2
    scratch += [dma((2 * nf,)), dma((2 * nf,))]
    scratch += [vmem(queries.shape, BF16), vmem((tok, depth), BF16), vmem(queries.shape, BF16),
                dma((5,))]
    out_shape = [
        jax.ShapeDtypeStruct(queries.shape, BF16),
        jax.ShapeDtypeStruct(queries.shape, BF16),
        jax.ShapeDtypeStruct((tok, width), BF16),
        jax.ShapeDtypeStruct((rows, cols), F32),
        jax.ShapeDtypeStruct((rows, cols), F32),
    ]
    spec = pl.BlockSpec(memory_space=pltpu.VMEM)
    whole = pl.BlockSpec(memory_space=pl.ANY)
    results = pl.pallas_call(
        functools.partial(kernel, (n, nf, exchange)),
        out_shape=[pltpu.VMEM(o.shape, o.dtype) for o in out_shape],
        in_specs=[whole] * 5 + [spec] * (len(operands) - 5),
        out_specs=[spec] * len(out_shape),
        scratch_shapes=scratch,
        compiler_params=pltpu.CompilerParams(
            collective_id=0, has_side_effects=True, vmem_limit_bytes=60 * 1024 * 1024),
    )(*operands)
    return tuple(pl.pallas_call(
        publish,
        out_shape=out_shape,
        in_specs=[spec] * len(out_shape),
        out_specs=[whole] * len(out_shape),
        scratch_shapes=[dma((len(out_shape),))],
        compiler_params=pltpu.CompilerParams(vmem_limit_bytes=8 * 1024 * 1024),
    )(*results))


def solution(mesh):
    placed = (
        P("seq", "fsdp"),
        P("seq", None),
        P("seq", "fsdp"),
        P("seq", "fsdp"),
        P("seq", "fsdp"),
    )
    return jax.shard_map(
        functools.partial(body, mesh.shape["seq"], mesh.shape["fsdp"]),
        mesh=mesh,
        in_specs=placed,
        out_specs=(P("seq", "fsdp"),) * 5,
        check_vma=False,
    )
```

```python
import functools
import math

import jax
import jax.numpy as jnp
import numpy as np
from jax import lax
from jax.experimental import pallas as pl
from jax.experimental.pallas import tpu as pltpu
from jax.sharding import PartitionSpec as P

HD = 128
ROPE_BASE = 500000.0
NEG = -1e30
MESH = pl.DeviceIdType.MESH
F32 = jnp.float32
BF16 = jnp.bfloat16


def loop(low, high, step):
    def run(i, carry):
        step(i)
        return carry

    lax.fori_loop(low, high, run, 0)


def dot_nn(a, b):
    return lax.dot_general(a, b, (((1,), (0,)), ((), ())), preferred_element_type=F32)


def dot_nt(a, b):
    return lax.dot_general(a, b, (((1,), (1,)), ((), ())), preferred_element_type=F32)


def dot_tn(a, b):
    return lax.dot_general(a, b, (((0,), (0,)), ((), ())), preferred_element_type=F32)


def block_of(ref, b, size):
    return ref.at[pl.ds(pl.multiple_of(b * size, size), size)]


def pieces_of(rows, inner):
    late = rows * 2 // 3 // 16 * 16 if inner == 2 else 0
    return [(0, rows - late, False)] + ([(rows - late, late, True)] if late else [])


def kernel(cfg, *refs):
    n, nf, exchange = cfg
    q_hbm, x_hbm, wk_ref, wv_ref, g_hbm, freq_ref = refs[:6]
    refs = refs[6:]
    if not exchange:
        xt_in = refs[0]
        refs = refs[1:]
    ao_ref, gq_ref, gi_ref, gwk_ref, gwv_ref = refs[:5]
    (wk_all, wv_all, k_all, v_all, dk_all, dv_all, x_all, q_st, g_st, g_tr,
     s_scr, p_scr, ds_scr, m_scr, l_scr, o_acc, dq_acc, dkp, dvp,
     rk_send, rk_recv, rv_send, rv_recv, own_dk, own_dv, sent_dk, sent_dv, cos_scr, sin_scr,
     gi_send, gi_recv, gi_own,
     wk_s, wk_r, wv_s, wv_r, k_s, k_r, v_s, v_r, dk_s, dk_r, dv_s, dv_r,
     x_s, x_r, xf_s, xf_r, rk_s, rk_r, rv_s, rv_r, gi_s, gi_r,
     q_ref, x_ref, g_ref, in_s) = refs[5:]
    tok = x_ref.shape[0]
    rows, cols = wk_ref.shape
    group = q_ref.shape[1] // cols
    m_cols = group * tok
    part = rows // nf
    width = gi_ref.shape[1]
    total = n * tok
    span = ds_scr.shape[0]
    spans = total // span
    per_span = span // tok
    chunk = math.gcd(span, 256)
    scale = HD ** (-0.5)
    s = lax.axis_index("seq")
    f = lax.axis_index("fsdp")
    inner = 2 if n % 2 == 0 else 1
    outer = n // inner
    z = s // inner
    y = s % inner
    mate = z * inner + (inner - 1 - y)

    def copy(src, dst, send, recv, dev):
        return pltpu.make_async_remote_copy(
            src_ref=src, dst_ref=dst, send_sem=send, recv_sem=recv, device_id=dev,
            device_id_type=MESH,
        )

    barrier = pltpu.get_barrier_semaphore()

    def greet(b):
        pl.semaphore_signal(barrier, inc=1, device_id=(b, f), device_id_type=MESH)

    def greet_fsdp(d):
        pl.semaphore_signal(
            barrier, inc=1, device_id=(s, (f + d) % nf), device_id_type=MESH)

    pl.when(z < outer - 1)(lambda: greet(s + inner))
    pl.when(z > 0)(lambda: greet(s - inner))
    if inner == 2:
        greet(mate)
    loop(1, nf, greet_fsdp)
    loads = [
        pltpu.make_async_copy(src, dst, in_s.at[i])
        for i, (src, dst) in enumerate((
            (wk_ref, block_of(wk_all, s, rows)), (wv_ref, block_of(wv_all, s, rows)),
            (x_hbm, x_ref), (q_hbm, q_ref), (g_hbm, g_ref)))
    ]
    for load in loads:
        load.start()

    def clear(b):
        at = pl.ds(pl.multiple_of(b * tok, tok), tok)
        k_all[at, :] = jnp.zeros((tok, cols), BF16)
        v_all[at, :] = jnp.zeros((tok, cols), BF16)

    loop(inner * (z + 1), n, clear)
    pl.semaphore_wait(
        barrier, jnp.minimum(z, 1) + jnp.minimum(outer - 1 - z, 1) + nf + inner - 2)

    class Gather:
        def __init__(self, ref, send, recv, causal=False):
            self.slot = lambda b: block_of(ref, b, tok)
            self.send, self.recv, self.causal = send, recv, causal

        def move(self, b, sem, level, row):
            ref = self.slot(b)
            return copy(ref, ref, self.send.at[sem], self.recv.at[b], (level * inner + row, f))

        def arrived(self, b):
            self.move(b, 0, z, y).wait_recv()

        def ends(self):
            return z == 0 if self.causal else jnp.logical_or(z == 0, z == outer - 1)

        def sends(self, act):
            if inner == 2:
                getattr(self.move(s, outer, z, 1 - y), act)()

            def near(d):
                def up():
                    getattr(self.move(s, z + d, z + d, y), act)()

                def down():
                    getattr(self.move(s, z - d, z - d, y), act)()

                pl.when(z + d < outer)(up)
                if not self.causal:
                    pl.when(z >= d)(down)

            loop(1, outer, near)
            if inner == 2 and outer > 1:
                pl.when(self.ends())(lambda: getattr(
                    self.move(s, z, outer - 1 - z, 1 - y), act)())

        def start(self):
            self.sends("start")

        def relay(self, act):
            def step(d):
                def pass_on(level):
                    b = level * inner + y
                    if act == "start":
                        self.arrived(b)
                    if inner == 2:
                        far = jnp.logical_or(level - z == outer - 1, z - level == outer - 1)
                        pl.when(jnp.logical_not(far))(lambda: getattr(
                            self.move(b, outer + 1 + level, z, 1 - y), act)())

                pl.when(z >= d)(lambda: pass_on(z - d))
                if not self.causal:
                    pl.when(z + d < outer)(lambda: pass_on(z + d))

            loop(1, outer, step)

        def forward(self):
            self.relay("start")

        def finish(self):
            if inner == 2:
                loop(0, z + 1 if self.causal else outer,
                     lambda level: self.arrived(level * inner + 1 - y))

        def drain(self):
            self.sends("wait_send")
            self.relay("wait_send")

    pieces = pieces_of(rows, inner)

    def is_end(level):
        return jnp.logical_or(level == 0, level == outer - 1)

    class Weights:
        def __init__(self, ref, send, recv):
            self.ref, self.send, self.recv = ref, send, recv

        def hop(self, q, b, way):
            at, count, late = pieces[q]
            ref = self.ref.at[pl.ds(pl.multiple_of(b * rows + at, 16), count)]
            dev = ((z + 1) * inner + y, (z - 1) * inner + y, mate)[way]
            if late:
                sem = 3 * outer + (2 * n + b // inner if way == 2 else way * n + b)
            else:
                sem = way * outer + b // inner
            return copy(ref, ref, self.send.at[sem], self.recv.at[q * n + b], (dev, f))

        def arrived(self, q, b):
            self.hop(q, b, 2).wait_recv()

        def own(self, q, way, act):
            def go():
                getattr(self.hop(q, s, way), act)()

            if way == 0:
                pl.when(z < outer - 1)(go)
            elif way == 1:
                pl.when(z > 0)(go)
            elif inner == 2:
                go()

        def mates(self, act):
            for q, (_, _, late) in enumerate(pieces):
                if late:
                    @pl.when(is_end(z))
                    def _(q=q):
                        if act == "start":
                            self.arrived(q, mate)
                        pl.when(z < outer - 1)(lambda: getattr(self.hop(q, mate, 0), act)())
                        pl.when(z > 0)(lambda: getattr(self.hop(q, mate, 1), act)())

        def relay(self, q, d, act):
            late = pieces[q][2]

            def one(b, way, to_mate):
                more = z < outer - 1 if way == 0 else z > 0
                if act == "start":
                    self.arrived(q, b)
                pl.when(more)(lambda: getattr(self.hop(q, b, way), act)())
                if to_mate:
                    getattr(self.hop(q, b, 2), act)()

            def pass_on(level, way):
                if late:
                    end = is_end(level)

                    @pl.when(end)
                    def _():
                        for line in range(inner):
                            one(level * inner + line, way, False)

                    pl.when(jnp.logical_not(end))(lambda: one(level * inner + y, way, True))
                else:
                    one(level * inner + y, way, inner == 2)

            pl.when(z >= d)(lambda: pass_on(z - d, 0))
            pl.when(z + d < outer)(lambda: pass_on(z + d, 1))

        def finish(self):
            if inner == 2:
                def step(level):
                    for q, (_, _, late) in enumerate(pieces):
                        def go(q=q):
                            self.arrived(q, level * inner + (1 - y))

                        if late:
                            pl.when(jnp.logical_not(is_end(level)))(go)
                        else:
                            go()

                loop(0, outer, step)

    def move_weights(act):
        gathers = (wk_gather, wv_gather)
        last = len(pieces) - 1
        for way in (0, 1):
            for gather in gathers:
                for q in range(len(pieces)):
                    gather.own(q, way, act)
        for q in range(last, -1, -1):
            for gather in gathers:
                gather.own(q, 2, act)

    def relay_weights(act):
        gathers = (wk_gather, wv_gather)
        for gather in gathers:
            gather.mates(act)

        def step(d):
            for q in range(len(pieces)):
                for gather in gathers:
                    gather.relay(q, d, act)

        loop(1, outer, step)

    wk_gather = Weights(wk_all, wk_s, wk_r)
    wv_gather = Weights(wv_all, wv_s, wv_r)
    k_gather = Gather(k_all, k_s, k_r, causal=True)
    v_gather = Gather(v_all, v_s, v_r, causal=True)
    dk_gather = Gather(dk_all, dk_s, dk_r)
    dv_gather = Gather(dv_all, dv_s, dv_r)

    loads[0].wait()
    loads[1].wait()
    move_weights("start")
    for load in loads[2:]:
        load.wait()

    own_rows = pl.ds(pl.multiple_of(s * tok, tok), tok)
    if exchange:
        own_part = pl.ds(pl.multiple_of(f * part, 128), part)

        def x_src(b):
            return x_ref.at[:, pl.ds(pl.multiple_of(b * rows + f * part, 128), part)]

        def x_slot(b, at):
            return x_all.at[pl.ds(pl.multiple_of(b * tok, tok), tok), at]

        def x_copy(b):
            return copy(x_src(b), x_slot(s, own_part), x_s.at[b], x_r.at[s], (b, f))

        def x_arrived(b):
            copy(x_src(b), x_slot(b, own_part), x_s.at[b], x_r.at[b], (b, f)).wait_recv()

        def xf_copy(d):
            ref = x_all.at[:, own_part]
            return copy(ref, ref, xf_s.at[d], xf_r.at[f], (s, (f + d) % nf))

        def xf_arrived(d):
            b = (f + d) % nf
            ref = x_all.at[:, pl.ds(pl.multiple_of(b * part, 128), part)]
            copy(ref, ref, xf_s.at[d], xf_r.at[b], (s, b)).wait_recv()

        x_all[own_rows, own_part] = x_ref[
            :, pl.ds(pl.multiple_of(s * rows + f * part, 128), part)]

    for g in range(group):
        at = slice(g * tok, (g + 1) * tok)
        q_st[at, :] = q_ref[:, g * HD:(g + 1) * HD]
        up = g_ref[:, g * HD:(g + 1) * HD]
        g_st[at, :] = up
        g_tr[:, at] = up.astype(F32).T
    lane = lax.broadcasted_iota(jnp.int32, (tok, HD), 1)
    position = (s * tok + lax.broadcasted_iota(jnp.int32, (tok, HD), 0)).astype(F32)
    angle = position * freq_ref[...]
    cos_scr[...] = jnp.cos(angle)
    sin_scr[...] = jnp.where(lane < HD // 2, -jnp.sin(angle), jnp.sin(angle))

    relay_weights("start")
    wk_gather.finish()

    lin = dot_nn(x_ref[...], wk_all[...])
    turned = lin * cos_scr[...] + pltpu.roll(lin, HD // 2, 1) * sin_scr[...]
    k_all[own_rows, :] = turned.astype(BF16)
    k_gather.start()

    if exchange:
        loop(0, s, lambda b: x_copy(b).start())
    wv_gather.finish()
    v_all[own_rows, :] = dot_nn(x_ref[...], wv_all[...]).astype(BF16)
    v_gather.start()
    k_gather.forward()
    v_gather.forward()
    k_gather.finish()
    def each_span(step):
        if spans == 1:
            step(0)
        else:
            loop(0, s * tok // span + 1, lambda i: step(pl.multiple_of(i * span, span)))

    def at_chunk(base, c):
        return pl.ds(base + c * chunk, chunk)

    def fold(value):
        return value.reshape(chunk // 8, 8, m_cols)

    column = jnp.concatenate(
        [lax.broadcasted_iota(jnp.int32, (chunk, tok), 1)] * group, axis=1)
    ahead = lax.broadcasted_iota(jnp.int32, (chunk, m_cols), 0) - column

    m_scr[...] = jnp.full(m_scr.shape, NEG, F32)
    l_scr[...] = jnp.zeros(l_scr.shape, F32)
    o_acc[...] = jnp.zeros(o_acc.shape, F32)
    dq_acc[...] = jnp.zeros(dq_acc.shape, F32)

    def score(base):
        for c in range(span // chunk):
            sc = dot_nt(k_all[at_chunk(base, c), :], q_st[...])
            sc = jnp.where(ahead <= s * tok - base - c * chunk, sc, NEG)
            s_scr[at_chunk(base, c), :] = sc
            m_scr[...] = jnp.maximum(m_scr[...], jnp.max(fold(sc), axis=0))

    each_span(score)
    top = jnp.max(m_scr[...], axis=0, keepdims=True)

    def weigh(base):
        for c in range(span // chunk):
            e = jnp.exp2((s_scr[at_chunk(base, c), :] - top) * (scale * math.log2(math.e)))
            s_scr[at_chunk(base, c), :] = e
            l_scr[...] += jnp.sum(fold(e), axis=0)

    each_span(weigh)
    inverse = 1.0 / jnp.sum(l_scr[...], axis=0, keepdims=True)

    half = n // 2 if n % 2 == 0 else 0
    low_end = s // half * half if half else 0

    class Reduce:
        def __init__(self, send, recv, send_sem, recv_sem, own, sent):
            self.send, self.recv, self.send_sem, self.recv_sem = send, recv, send_sem, recv_sem
            self.own, self.sent = own, sent

        def direct(self, j):
            return copy(self.send.at[j], self.recv.at[s], self.send_sem.at[j], self.recv_sem.at[s],
                        (j, f))

        def inward(self, j):
            slot = n + s - half
            return copy(self.send.at[j], self.recv.at[slot], self.send_sem.at[j],
                        self.recv_sem.at[slot], (j + half, f))

        def got(self, slot):
            copy(self.send.at[0], self.recv.at[slot], self.send_sem.at[0], self.recv_sem.at[slot],
                 (mate, f)).wait_recv()
            return self.recv[slot].astype(F32)

        def hand(self, low, high, act):
            high = jnp.minimum(high, s)
            loop(jnp.maximum(low, low_end), high, lambda j: getattr(self.direct(j), act)())
            if half:
                @pl.when(s >= half)
                def _():
                    loop(low, jnp.minimum(high, half), lambda j: pl.when(j + half != s)(
                        lambda: getattr(self.inward(j), act)()))

        def pass_on(self):
            if half:
                @pl.when(s >= half)
                def _():
                    def add(i):
                        self.sent[...] += self.got(n + i - half)

                    loop(half, s, add)
                    loop(s + 1, n, add)
                    self.send[s - half] = self.sent[...].astype(BF16)
                    self.direct(s - half).start()

        def take(self):
            def add(j):
                self.own[...] += self.got(j)

            loop(s + 1, low_end + half if half else n, add)
            if half:
                pl.when(s < half)(lambda: add(s + half))

        def drain(self):
            self.hand(0, n, "wait_send")
            if half:
                pl.when(s >= half)(lambda: self.direct(s - half).wait_send())

    rk = Reduce(rk_send, rk_recv, rk_s, rk_r, own_dk, sent_dk)
    rv = Reduce(rv_send, rv_recv, rv_s, rv_r, own_dv, sent_dv)

    def hand_out(base, low, high, partial, reduce):
        first = base // tok
        reduce.hand(first + low, first + high, "start")

        def keep(block, out):
            at = pl.ds(pl.multiple_of((block - first) * tok, tok), tok)
            out[...] = partial[at, :]

        if spans == 1:
            if high == per_span:
                keep(s, reduce.own)
                if half:
                    pl.when(s >= half)(lambda: keep(s - half, reduce.sent))
        else:
            for block, out in ((s, reduce.own), (s - half, reduce.sent)):
                @pl.when(jnp.logical_and(block >= first + low, block < first + high))
                def _(block=block, out=out):
                    keep(block, out)

    def store_parts(base, c, value, partial, send):
        partial[c * chunk:(c + 1) * chunk, :] = value
        for i in range(chunk // tok):
            send[base // tok + c * (chunk // tok) + i] = value[i * tok:(i + 1) * tok].astype(BF16)

    def value_part(base):
        for c in range(span // chunk):
            p = s_scr[at_chunk(base, c), :] * inverse
            s_scr[at_chunk(base, c), :] = p
            low = p.astype(BF16)
            p_scr[at_chunk(base, c), :] = low
            store_parts(base, c, dot_nn(low, g_st[...]), dvp, rv_send)
        hand_out(base, 0, per_span, dvp, rv)

    each_span(value_part)
    v_gather.finish()

    def weighted(base):
        o_acc[...] += dot_tn(v_all[pl.ds(base, span), :], p_scr[pl.ds(base, span), :])

    each_span(weighted)
    delta = jnp.sum(g_tr[...] * o_acc[...], axis=0, keepdims=True)

    def key_part(base):
        halves = 2 if (span // chunk) % 2 == 0 else 1
        count = span // chunk // halves
        for part_of in range(halves):
            for c in range(part_of * count, (part_of + 1) * count):
                dp = dot_nt(v_all[at_chunk(base, c), :], g_st[...])
                ds = (s_scr[at_chunk(base, c), :] * (dp - delta)).astype(BF16)
                ds_scr[c * chunk:(c + 1) * chunk, :] = ds
                store_parts(base, c, dot_nn(ds, q_st[...]), dkp, rk_send)
            hand_out(base, part_of * per_span // halves, (part_of + 1) * per_span // halves, dkp, rk)
        dq_acc[...] += dot_tn(k_all[pl.ds(base, span), :], ds_scr[...])

    each_span(key_part)
    for g in range(group):
        at = slice(g * tok, (g + 1) * tok)
        ao_ref[:, g * HD:(g + 1) * HD] = o_acc[:, at].T.astype(BF16)
        gq_ref[:, g * HD:(g + 1) * HD] = (dq_acc[:, at] * scale).T.astype(BF16)

    if exchange:
        loop(s + 1, n, lambda b: x_copy(b).start())

    rv.pass_on()
    rv.take()
    dv_all[own_rows, :] = own_dv[...].astype(BF16)
    dv_gather.start()
    rk.pass_on()
    if exchange:
        loop(0, s, x_arrived)
        loop(s + 1, n, x_arrived)
        loop(1, nf, lambda d: xf_copy(d).start())
    rk.take()
    lin = own_dk[...] * scale
    turned = lin * cos_scr[...] - pltpu.roll(lin, HD // 2, 1) * sin_scr[...]
    dk_all[own_rows, :] = turned.astype(BF16)
    dk_gather.start()
    dv_gather.forward()

    def input_term(b):
        at = pl.ds(pl.multiple_of(b * width, width), width)
        return (dot_nt(dk_all[own_rows, :], wk_all[at, :])
                + dot_nt(dv_all[own_rows, :], wv_all[at, :]))

    cores = 2 if nf % 2 == 0 else 1
    chips = nf // cores
    chip = f // cores
    core = f % cores
    twin = chip * cores + (cores - 1 - core)

    def gi_twin(o):
        return copy(gi_send.at[o], gi_recv.at[o], gi_s.at[o], gi_r.at[o], (s, twin))

    def gi_far(d):
        return copy(gi_send.at[chips + d], gi_recv.at[chips + chip], gi_s.at[chips + d],
                    gi_r.at[chips + chip], (s, (chip + d) % chips * cores + core))

    def twin_term(d):
        o = (chip + d) % chips
        gi_send[o] = input_term(o * cores + 1 - core).astype(BF16)
        gi_twin(o).start()

    def own_term(d):
        o = (chip + d) % chips
        gi_own[o] = input_term(o * cores + core)

    def join(d):
        o = (chip + d) % chips
        gi_twin(o).wait_recv()
        gi_own[o] += gi_recv[o].astype(F32)

    def far_term(d):
        if cores == 2:
            join(d)
        gi_send[chips + d] = gi_own[(chip + d) % chips].astype(BF16)
        gi_far(d).start()

    def far_terms(d):
        if cores == 2:
            twin_term(d)
        own_term(d)
        far_term(d)

    loop(1, chips, far_terms)
    if cores == 2:
        twin_term(0)
    own_term(0)

    def weight_grad(grads, out):
        if exchange:
            out[...] = dot_tn(grads[...], x_all[...]).T
        else:
            grad = None
            step = min(total, 1024)
            for at in range(0, total, step):
                term = dot_tn(xt_in[at:at + step, :], grads[at:at + step, :])
                grad = term if grad is None else grad + term
            out[...] = grad

    dk_gather.forward()
    dv_gather.finish()
    if exchange:
        loop(1, nf, xf_arrived)
    weight_grad(dv_all, gwv_ref)
    dk_gather.finish()
    weight_grad(dk_all, gwk_ref)

    def gi_take(d):
        b = (chip + d) % chips
        copy(gi_send.at[chips + d], gi_recv.at[chips + b], gi_s.at[chips + d],
             gi_r.at[chips + b], (s, b * cores + core)).wait_recv()
        gi_own[chip] += gi_recv[chips + b].astype(F32)

    if cores == 2:
        join(0)
    loop(1, chips, gi_take)
    gi_ref[...] = gi_own[chip].astype(BF16)

    move_weights("wait_send")
    relay_weights("wait_send")
    for gather in (k_gather, v_gather, dk_gather, dv_gather):
        gather.drain()
    if exchange:
        loop(0, s, lambda b: x_copy(b).wait_send())
        loop(s + 1, n, lambda b: x_copy(b).wait_send())
        loop(1, nf, lambda d: xf_copy(d).wait_send())
    rv.drain()
    rk.drain()
    if cores == 2:
        loop(0, chips, lambda o: gi_twin(o).wait_send())
    loop(1, chips, lambda d: gi_far(d).wait_send())


def publish(*refs):
    count = len(refs) // 2
    sems = refs[-1]
    moves = [pltpu.make_async_copy(refs[i], refs[count + i], sems.at[i]) for i in range(count)]
    for move in moves:
        move.start()
    for move in moves:
        move.wait()


def body(n, nf, queries, layer_input, w_key, w_value, grad_out):
    tok, depth = layer_input.shape
    rows, cols = w_key.shape
    assert cols == HD
    group = queries.shape[1] // cols
    m_cols = group * tok
    part = rows // nf
    exchange = part % 128 == 0
    half = HD // 2
    freq = np.float32(ROPE_BASE) ** (-(np.arange(half, dtype=np.float32) * np.float32(2.0 / HD)))
    freq = jnp.asarray(np.concatenate([freq, freq])[None, :], F32)
    operands = [queries, layer_input, w_key, w_value, grad_out, freq]
    if not exchange:
        operands.append(
            lax.all_to_all(layer_input, "seq", split_axis=1, concat_axis=0, tiled=True))
    width = depth // nf
    total = n * tok
    span = math.gcd(total, 1024)
    inner = 2 if n % 2 == 0 else 1
    outer = n // inner
    pieces = len(pieces_of(rows, inner))
    hops = 3 * outer + (2 * n + outer if pieces > 1 else 0)
    vmem = pltpu.VMEM
    dma = pltpu.SemaphoreType.DMA
    scratch = [vmem((depth, cols), BF16)] * 2
    scratch += [vmem((total, cols), BF16)] * 4
    scratch += [
        vmem((total, rows) if exchange else (16, 128), BF16),
        vmem((m_cols, HD), BF16), vmem((m_cols, HD), BF16), vmem((HD, m_cols), F32),
        vmem((total, m_cols), F32), vmem((total, m_cols), BF16), vmem((span, m_cols), BF16),
        vmem((8, m_cols), F32), vmem((8, m_cols), F32),
        vmem((HD, m_cols), F32), vmem((HD, m_cols), F32),
        vmem((span, cols), F32), vmem((span, cols), F32),
    ]
    slots = n + n // 2
    scratch += [vmem((n, tok, cols), BF16), vmem((slots, tok, cols), BF16)] * 2
    scratch += [vmem((tok, cols), F32)] * 6
    scratch += [
        vmem((2 * nf, tok, width), BF16), vmem((2 * nf, tok, width), BF16),
        vmem((nf, tok, width), F32),
    ]
    scratch += [dma((hops,)), dma((pieces * n,))] * 2
    scratch += [dma((2 * outer + 1,)), dma((n,))] * 4
    scratch += [dma((n,)), dma((n,)), dma((nf,)), dma((nf,))]
    scratch += [dma((n,)), dma((slots,))] * 2
    scratch += [dma((2 * nf,)), dma((2 * nf,))]
    scratch += [vmem(queries.shape, BF16), vmem((tok, depth), BF16), vmem(queries.shape, BF16),
                dma((5,))]
    out_shape = [
        jax.ShapeDtypeStruct(queries.shape, BF16),
        jax.ShapeDtypeStruct(queries.shape, BF16),
        jax.ShapeDtypeStruct((tok, width), BF16),
        jax.ShapeDtypeStruct((rows, cols), F32),
        jax.ShapeDtypeStruct((rows, cols), F32),
    ]
    spec = pl.BlockSpec(memory_space=pltpu.VMEM)
    whole = pl.BlockSpec(memory_space=pl.ANY)
    results = pl.pallas_call(
        functools.partial(kernel, (n, nf, exchange)),
        out_shape=[pltpu.VMEM(o.shape, o.dtype) for o in out_shape],
        in_specs=[whole] * 5 + [spec] * (len(operands) - 5),
        out_specs=[spec] * len(out_shape),
        scratch_shapes=scratch,
        compiler_params=pltpu.CompilerParams(
            collective_id=0, has_side_effects=True, vmem_limit_bytes=60 * 1024 * 1024),
    )(*operands)
    return tuple(pl.pallas_call(
        publish,
        out_shape=out_shape,
        in_specs=[spec] * len(out_shape),
        out_specs=[whole] * len(out_shape),
        scratch_shapes=[dma((len(out_shape),))],
        compiler_params=pltpu.CompilerParams(vmem_limit_bytes=8 * 1024 * 1024),
    )(*results))


def solution(mesh):
    placed = (
        P("seq", "fsdp"),
        P("seq", None),
        P("seq", "fsdp"),
        P("seq", "fsdp"),
        P("seq", "fsdp"),
    )
    return jax.shard_map(
        functools.partial(body, mesh.shape["seq"], mesh.shape["fsdp"]),
        mesh=mesh,
        in_specs=placed,
        out_specs=(P("seq", "fsdp"),) * 5,
        check_vma=False,
    )
```

```python
import functools
import math

import jax
import jax.numpy as jnp
import numpy as np
from jax import lax
from jax.experimental import pallas as pl
from jax.experimental.pallas import tpu as pltpu
from jax.sharding import PartitionSpec as P

HD = 128
ROPE_BASE = 500000.0
NEG = -1e30
MESH = pl.DeviceIdType.MESH
F32 = jnp.float32
BF16 = jnp.bfloat16


def loop(low, high, step):
    def run(i, carry):
        step(i)
        return carry

    lax.fori_loop(low, high, run, 0)


def dot_nn(a, b):
    return lax.dot_general(a, b, (((1,), (0,)), ((), ())), preferred_element_type=F32)


def dot_nt(a, b):
    return lax.dot_general(a, b, (((1,), (1,)), ((), ())), preferred_element_type=F32)


def dot_tn(a, b):
    return lax.dot_general(a, b, (((0,), (0,)), ((), ())), preferred_element_type=F32)


def block_of(ref, b, size):
    return ref.at[pl.ds(pl.multiple_of(b * size, size), size)]


def pieces_of(rows, inner):
    late = rows * 5 // 8 // 16 * 16 if inner == 2 else 0
    return [(0, rows - late, False)] + ([(rows - late, late, True)] if late else [])


def kernel(cfg, *refs):
    n, nf, exchange = cfg
    q_hbm, x_hbm, wk_ref, wv_ref, g_hbm, freq_ref = refs[:6]
    refs = refs[6:]
    if not exchange:
        xt_in = refs[0]
        refs = refs[1:]
    ao_ref, gq_ref, gi_ref, gwk_ref, gwv_ref = refs[:5]
    (wk_all, wv_all, k_all, v_all, dk_all, dv_all, x_all, q_st, g_st, g_tr,
     s_scr, p_scr, ds_scr, m_scr, l_scr, o_acc, dq_acc, dkp, dvp,
     rk_send, rk_recv, rv_send, rv_recv, own_dk, own_dv, sent_dk, sent_dv, cos_scr, sin_scr,
     gi_send, gi_recv, gi_own, xg, pe_send, pe_recv,
     told, xe_s, xe_r, pe_s, pe_r, wk_s, wk_r, wv_s, wv_r, k_s, k_r, v_s, v_r, dk_s, dk_r, dv_s, dv_r,
     x_s, x_r, xf_s, xf_r, rk_s, rk_r, rv_s, rv_r, gi_s, gi_r,
     q_ref, x_ref, g_ref, in_s) = refs[5:]
    tok = x_ref.shape[0]
    rows, cols = wk_ref.shape
    group = q_ref.shape[1] // cols
    m_cols = group * tok
    part = rows // nf
    width = gi_ref.shape[1]
    total = n * tok
    span = ds_scr.shape[0]
    spans = total // span
    per_span = span // tok
    chunk = math.gcd(span, 256)
    scale = HD ** (-0.5)
    s = lax.axis_index("seq")
    f = lax.axis_index("fsdp")
    inner = 2 if n % 2 == 0 else 1
    outer = n // inner
    z = s // inner
    y = s % inner
    mate = z * inner + (inner - 1 - y)
    last = outer - 1
    hosted = exchange and inner == 2 and outer >= 4
    cores = 2 if nf % 2 == 0 else 1
    chips = nf // cores
    chip = f // cores
    core = f % cores
    twin = chip * cores + (cores - 1 - core)

    def copy(src, dst, send, recv, dev):
        return pltpu.make_async_remote_copy(
            src_ref=src, dst_ref=dst, send_sem=send, recv_sem=recv, device_id=dev,
            device_id_type=MESH,
        )

    barrier = pltpu.get_barrier_semaphore()

    def greet(b):
        pl.semaphore_signal(barrier, inc=1, device_id=(b, f), device_id_type=MESH)

    def greet_fsdp(d):
        pl.semaphore_signal(
            barrier, inc=1, device_id=(s, (f + d) % nf), device_id_type=MESH)

    pl.when(z < outer - 1)(lambda: greet(s + inner))
    pl.when(z > 0)(lambda: greet(s - inner))
    if inner == 2:
        greet(mate)
    loop(1, nf, greet_fsdp)
    loads = [
        pltpu.make_async_copy(src, dst, in_s.at[i])
        for i, (src, dst) in enumerate((
            (wk_ref, block_of(wk_all, s, rows)), (wv_ref, block_of(wv_all, s, rows)),
            (x_hbm, x_ref), (q_hbm, q_ref), (g_hbm, g_ref)))
    ]
    for load in loads:
        load.start()

    def clear(b):
        at = pl.ds(pl.multiple_of(b * tok, tok), tok)
        k_all[at, :] = jnp.zeros((tok, cols), BF16)
        v_all[at, :] = jnp.zeros((tok, cols), BF16)

    loop(inner * (z + 1), n, clear)
    pl.semaphore_wait(
        barrier, jnp.minimum(z, 1) + jnp.minimum(outer - 1 - z, 1) + nf + inner - 2)

    class Gather:
        def __init__(self, ref, send, recv, causal=False):
            self.slot = lambda b: block_of(ref, b, tok)
            self.send, self.recv, self.causal = send, recv, causal

        def move(self, b, sem, level, row):
            ref = self.slot(b)
            return copy(ref, ref, self.send.at[sem], self.recv.at[b], (level * inner + row, f))

        def arrived(self, b):
            self.move(b, 0, z, y).wait_recv()

        def ends(self):
            return z == 0 if self.causal else jnp.logical_or(z == 0, z == outer - 1)

        def sends(self, act):
            def run(sem, level, row):
                getattr(self.move(s, sem, level, row), act)()

            def near(d):
                pl.when(z + d < outer)(lambda: run(z + d, z + d, y))
                if not self.causal:
                    pl.when(z >= d)(lambda: run(z - d, z - d, y))

            def far():
                if inner == 2 and outer > 1:
                    pl.when(self.ends())(lambda: run(z, outer - 1 - z, 1 - y))

            def to_mate():
                if inner == 2:
                    run(outer, z, 1 - y)

            if self.causal:
                far()
                loop(0, outer - 1, lambda i: near(outer - 1 - i))
                to_mate()
            else:
                to_mate()
                loop(1, outer, near)
                far()

        def start(self):
            self.sends("start")

        def relay(self, act, low=1, high=outer):
            def step(d):
                def pass_on(level):
                    b = level * inner + y
                    if act == "start":
                        self.arrived(b)
                    if inner == 2:
                        far = jnp.logical_or(level - z == outer - 1, z - level == outer - 1)
                        pl.when(jnp.logical_not(far))(lambda: getattr(
                            self.move(b, outer + 1 + level, z, 1 - y), act)())

                pl.when(z >= d)(lambda: pass_on(z - d))
                if not self.causal:
                    pl.when(z + d < outer)(lambda: pass_on(z + d))

            loop(low, high, step)

        def forward(self, low=1, high=outer):
            self.relay("start", low, high)

        def finish(self):
            if inner == 2:
                loop(0, z + 1 if self.causal else outer,
                     lambda level: self.arrived(level * inner + 1 - y))

        def drain(self):
            self.sends("wait_send")
            self.relay("wait_send")

    pieces = pieces_of(rows, inner)

    def is_end(level):
        return jnp.logical_or(level == 0, level == outer - 1)

    class Weights:
        def __init__(self, ref, send, recv, deferred=False):
            self.ref, self.send, self.recv, self.deferred = ref, send, recv, deferred

        def hop(self, q, b, way):
            at, count, late = pieces[q]
            ref = self.ref.at[pl.ds(pl.multiple_of(b * rows + at, 16), count)]
            dev = ((z + 1) * inner + y, (z - 1) * inner + y, mate)[way]
            if late:
                sem = 3 * outer + (2 * n + b // inner if way == 2 else way * n + b)
            else:
                sem = way * outer + b // inner
            return copy(ref, ref, self.send.at[sem], self.recv.at[q * n + b], (dev, f))

        def arrived(self, q, b):
            self.hop(q, b, 2).wait_recv()

        def own(self, q, way, act):
            def go():
                getattr(self.hop(q, s, way), act)()

            if way == 0:
                pl.when(z < outer - 1)(go)
            elif way == 1:
                pl.when(z > 0)(go)
            elif inner == 2:
                go()

        def mates(self, act):
            for q, (_, _, late) in enumerate(pieces):
                if late:
                    @pl.when(is_end(z))
                    def _(q=q):
                        if act == "start":
                            self.arrived(q, mate)
                        pl.when(z < outer - 1)(lambda: getattr(self.hop(q, mate, 0), act)())
                        pl.when(z > 0)(lambda: getattr(self.hop(q, mate, 1), act)())

        def relay(self, q, d, act):
            late = pieces[q][2]

            def one(b, way, to_mate):
                more = z < last if way == 0 else z > 0
                if self.deferred:
                    more = jnp.logical_and(more, jnp.logical_not(
                        jnp.logical_and(z == last - 1, b // inner == 0) if way == 0
                        else jnp.logical_and(z == 1, b // inner == last)))
                if act == "start":
                    self.arrived(q, b)
                pl.when(more)(lambda: getattr(self.hop(q, b, way), act)())
                if to_mate:
                    getattr(self.hop(q, b, 2), act)()

            def pass_on(level, way):
                if late:
                    end = is_end(level)

                    @pl.when(end)
                    def _():
                        for line in range(inner):
                            one(level * inner + line, way, False)

                    pl.when(jnp.logical_not(end))(lambda: one(level * inner + y, way, True))
                else:
                    one(level * inner + y, way, inner == 2)

            pl.when(z >= d)(lambda: pass_on(z - d, 0))
            pl.when(z + d < outer)(lambda: pass_on(z + d, 1))

        def held(self, way, act):
            def run():
                for q, (_, _, late) in enumerate(pieces):
                    for line in range(inner) if late else (y,):
                        level = last if way == 1 else 0
                        getattr(self.hop(q, level * inner + line, way), act)()

            pl.when(z == (1 if way == 1 else last - 1))(run)

        def finish(self, low=0, high=outer):
            if inner == 2:
                def step(level):
                    for q, (_, _, late) in enumerate(pieces):
                        def go(q=q):
                            self.arrived(q, level * inner + (1 - y))

                        if late:
                            pl.when(jnp.logical_not(is_end(level)))(go)
                        else:
                            go()

                loop(low, high, step)

    def move_weights(act):
        for gather in (wk_gather, wv_gather):
            for q in range(len(pieces)):
                gather.own(q, 0, act)
                gather.own(q, 1, act)
            for q in range(len(pieces) - 1, -1, -1):
                gather.own(q, 2, act)
            gather.mates(act)

    def relay_weights(act, low, high):
        def step(d):
            for gather in (wk_gather, wv_gather):
                for q in range(len(pieces)):
                    gather.relay(q, d, act)

        loop(low, high, step)

    def when_host(act):
        pl.when(jnp.logical_or(z == 1, z == last - 1))(act)

    class Guest:
        def __init__(self):
            self.span = inner * rows
            self.part = self.span // nf

        def place(self, p):
            return xg.at[:, pl.ds(pl.multiple_of(p * self.part, 128), self.part)]

        def move(self, p, sem, dev):
            return copy(self.place(p), self.place(p), xe_s.at[sem], xe_r.at[p], dev)

        def arrived(self, p):
            self.move(p, 0, (s, f)).wait_recv()

        def leave(self, act):
            @pl.when(is_end(z))
            def _():
                host = jnp.minimum(jnp.maximum(z, 1), last - 1) * inner + y
                at = pl.multiple_of((last - z) * self.span + f * self.part, 128)
                getattr(copy(x_ref.at[:, pl.ds(at, self.part)], self.place(f), xe_s.at[0],
                             xe_r.at[f], (host, f)), act)()

        def spread(self, act):
            def run():
                if act == "start":
                    self.arrived(f)
                loop(1, chips, lambda d: getattr(self.move(
                    f, d, (s, (chip + d) % chips * cores + core)), act)())
                if cores == 2:
                    getattr(self.move(f, chips + chip, (s, twin)), act)()

            when_host(run)

        def share(self, act):
            def step(d):
                o = (chip + d) % chips
                if act == "start":
                    self.arrived(o * cores + core)
                if cores == 2:
                    getattr(self.move(o * cores + core, chips + o, (s, twin)), act)()

            when_host(lambda: loop(1, chips, step))

        def finish(self):
            if cores == 2:
                loop(0, chips, lambda o: self.arrived(o * cores + 1 - core))

        def reply(self, i):
            end = jnp.minimum(z - 1, 1) * last
            return copy(pe_send.at[i], pe_recv.at[i], pe_s.at[i], pe_r.at[i], (end * inner + y, f))

        def partial(self, i, weights):
            def run():
                at = (last - jnp.minimum(z - 1, 1) * last) * self.span
                w = weights[pl.ds(pl.multiple_of(at, 16), self.span), :]
                pe_send[i] = dot_nn(xg[...], w).astype(BF16)
                self.reply(i).start()

            when_host(run)

        def rest(self, weights):
            at = pl.multiple_of(z // last * self.span, 128)
            here = pl.ds(at, (outer - 1) * self.span)
            return dot_nn(x_ref[:, here], weights[here, :])

        def returned(self, i):
            copy(pe_send.at[i], pe_recv.at[i], pe_s.at[i], pe_r.at[i], (mate, f)).wait_recv()
            return pe_recv[i].astype(F32)

        def drain(self):
            self.leave("wait_send")
            self.spread("wait_send")
            self.share("wait_send")
            when_host(lambda: loop(0, 2, lambda i: self.reply(i).wait_send()))

    wk_gather = Weights(wk_all, wk_s, wk_r)
    wv_gather = Weights(wv_all, wv_s, wv_r, deferred=hosted)
    guests = Guest() if hosted else None
    k_gather = Gather(k_all, k_s, k_r, causal=True)
    v_gather = Gather(v_all, v_s, v_r, causal=True)
    dk_gather = Gather(dk_all, *((v_s, v_r) if exchange else (dk_s, dk_r)))
    dv_gather = Gather(dv_all, *((k_s, k_r) if exchange else (dv_s, dv_r)))

    for load in loads[:3]:
        load.wait()
    if hosted:
        guests.leave("start")
    move_weights("start")
    for load in loads[3:]:
        load.wait()

    own_rows = pl.ds(pl.multiple_of(s * tok, tok), tok)
    if exchange:
        own_part = pl.ds(pl.multiple_of(f * part, 128), part)

        def x_src(b):
            return x_ref.at[:, pl.ds(pl.multiple_of(b * rows + f * part, 128), part)]

        def x_slot(b, at):
            return x_all.at[pl.ds(pl.multiple_of(b * tok, tok), tok), at]

        def x_copy(b):
            return copy(x_src(b), x_slot(s, own_part), x_s.at[b], x_r.at[s], (b, f))

        def x_arrived(b):
            copy(x_src(b), x_slot(b, own_part), x_s.at[b], x_r.at[b], (b, f)).wait_recv()

        def xf_copy(d):
            ref = x_all.at[:, own_part]
            return copy(ref, ref, xf_s.at[d], xf_r.at[f], (s, (f + d) % nf))

        def xf_arrived(d):
            b = (f + d) % nf
            ref = x_all.at[:, pl.ds(pl.multiple_of(b * part, 128), part)]
            copy(ref, ref, xf_s.at[d], xf_r.at[b], (s, b)).wait_recv()

        x_all[own_rows, own_part] = x_ref[
            :, pl.ds(pl.multiple_of(s * rows + f * part, 128), part)]

    for g in range(group):
        at = slice(g * tok, (g + 1) * tok)
        q_st[at, :] = q_ref[:, g * HD:(g + 1) * HD]
        up = g_ref[:, g * HD:(g + 1) * HD]
        g_st[at, :] = up
        g_tr[:, at] = up.astype(F32).T
    lane = lax.broadcasted_iota(jnp.int32, (tok, HD), 1)
    position = (s * tok + lax.broadcasted_iota(jnp.int32, (tok, HD), 0)).astype(F32)
    angle = position * freq_ref[...]
    cos_scr[...] = jnp.cos(angle)
    sin_scr[...] = jnp.where(lane < HD // 2, -jnp.sin(angle), jnp.sin(angle))

    def tell(which, device):
        pl.semaphore_signal(
            told.at[which], inc=1, device_id=(device, f), device_id_type=MESH)

    if hosted:
        pl.when(z < last - 1)(lambda: pl.semaphore_wait(told.at[0], 1))
        pl.when(jnp.logical_and(z > 0, z < last))(lambda: tell(0, s - inner))

        @pl.when(z == 0)
        def _():
            tell(1, mate)
            pl.semaphore_wait(told.at[1], 1)

    relay_weights("start", 1, 2)
    if hosted:
        guests.spread("start")
    relay_weights("start", 2, outer - 1)
    if hosted:
        guests.share("start")
    def x_ahead():
        loop(inner * (z + 1), n, lambda b: x_copy(b).start())

    if hosted:
        pl.when(z == 0)(x_ahead)

    def last_relays(act, gathers):
        for gather in gathers:
            for q in range(len(pieces)):
                gather.relay(q, outer - 1, act)

    def rotated(lin):
        return lin * cos_scr[...] + pltpu.roll(lin, HD // 2, 1) * sin_scr[...]

    def finish_levels(low, high):
        wk_gather.finish(low, high)
        wv_gather.finish(low, high)

    def keep_keys(lin):
        k_all[own_rows, :] = rotated(lin).astype(BF16)
        k_gather.start()

    def keep_values(value):
        v_all[own_rows, :] = value.astype(BF16)
        v_gather.start()

    def project():
        keep_keys(dot_nn(x_ref[...], wk_all[...]))
        keep_values(dot_nn(x_ref[...], wv_all[...]))

    def project_end():
        first = jnp.minimum(z, 1)
        with jax.named_scope("wkfin"):
            finish_levels(first, first + outer - 1)
        with jax.named_scope("kproj"):
            keys, values = guests.rest(wk_all), guests.rest(wv_all)
        with jax.named_scope("xfin"):
            keep_keys(keys + guests.returned(0))
        with jax.named_scope("vproj"):
            keep_values(values + guests.returned(1))

    def project_inner():
        with jax.named_scope("wkfin"):
            finish_levels(0, outer)
        with jax.named_scope("xfin"):
            pl.when(z < last - 1)(x_ahead)
            when_host(guests.finish)
        with jax.named_scope("kproj"):
            guests.partial(0, wk_all)
            guests.partial(1, wv_all)
        with jax.named_scope("vproj"):
            project()

    if hosted:
        pl.when(is_end(z))(project_end)
        pl.when(jnp.logical_not(is_end(z)))(project_inner)
    else:
        if outer > 1:
            last_relays("start", (wk_gather, wv_gather))
        finish_levels(0, outer)
        project()
    if hosted:
        wv_gather.held(1, "start")
    if exchange:
        pl.when(z == last - 1)(x_ahead) if hosted else x_ahead()
        loop(0, s, lambda b: x_copy(b).start())
    k_gather.forward()
    v_gather.forward()
    if hosted:
        last_relays("start", (wk_gather,))
    k_gather.finish()
    def each_span(step):
        if spans == 1:
            step(0)
        else:
            loop(0, s * tok // span + 1, lambda i: step(pl.multiple_of(i * span, span)))

    def at_chunk(base, c):
        return pl.ds(base + c * chunk, chunk)

    def fold(value):
        return value.reshape(chunk // 8, 8, m_cols)

    column = jnp.concatenate(
        [lax.broadcasted_iota(jnp.int32, (chunk, tok), 1)] * group, axis=1)
    ahead = lax.broadcasted_iota(jnp.int32, (chunk, m_cols), 0) - column

    m_scr[...] = jnp.full(m_scr.shape, NEG, F32)
    l_scr[...] = jnp.zeros(l_scr.shape, F32)
    o_acc[...] = jnp.zeros(o_acc.shape, F32)
    dq_acc[...] = jnp.zeros(dq_acc.shape, F32)

    def score(base):
        for c in range(span // chunk):
            sc = dot_nt(k_all[at_chunk(base, c), :], q_st[...])
            sc = jnp.where(ahead <= s * tok - base - c * chunk, sc, NEG)
            s_scr[at_chunk(base, c), :] = sc
            m_scr[...] = jnp.maximum(m_scr[...], jnp.max(fold(sc), axis=0))

    each_span(score)
    top = jnp.max(m_scr[...], axis=0, keepdims=True)

    def weigh(base):
        for c in range(span // chunk):
            e = jnp.exp2((s_scr[at_chunk(base, c), :] - top) * (scale * math.log2(math.e)))
            s_scr[at_chunk(base, c), :] = e
            l_scr[...] += jnp.sum(fold(e), axis=0)

    each_span(weigh)
    inverse = 1.0 / jnp.sum(l_scr[...], axis=0, keepdims=True)

    half = n // 2 if n % 2 == 0 else 0
    low_end = s // half * half if half else 0

    class Reduce:
        def __init__(self, send, recv, send_sem, recv_sem, own, sent):
            self.send, self.recv, self.send_sem, self.recv_sem = send, recv, send_sem, recv_sem
            self.own, self.sent = own, sent

        def direct(self, j):
            return copy(self.send.at[j], self.recv.at[s], self.send_sem.at[j], self.recv_sem.at[s],
                        (j, f))

        def inward(self, j):
            slot = n + s - half
            return copy(self.send.at[j], self.recv.at[slot], self.send_sem.at[j],
                        self.recv_sem.at[slot], (j + half, f))

        def got(self, slot):
            copy(self.send.at[0], self.recv.at[slot], self.send_sem.at[0], self.recv_sem.at[slot],
                 (mate, f)).wait_recv()
            return self.recv[slot].astype(F32)

        def hand(self, low, high, act):
            high = jnp.minimum(high, s)
            loop(jnp.maximum(low, low_end), high, lambda j: getattr(self.direct(j), act)())
            if half:
                @pl.when(s >= half)
                def _():
                    loop(low, jnp.minimum(high, half), lambda j: pl.when(j + half != s)(
                        lambda: getattr(self.inward(j), act)()))

        def pass_on(self):
            if half:
                @pl.when(s >= half)
                def _():
                    def add(i):
                        self.sent[...] += self.got(n + i - half)

                    loop(half, s, add)
                    loop(s + 1, n, add)
                    self.send[s - half] = self.sent[...].astype(BF16)
                    self.direct(s - half).start()

        def take(self):
            def add(j):
                self.own[...] += self.got(j)

            loop(s + 1, low_end + half if half else n, add)
            if half:
                pl.when(s < half)(lambda: add(s + half))

        def drain(self):
            self.hand(0, n, "wait_send")
            if half:
                pl.when(s >= half)(lambda: self.direct(s - half).wait_send())

    rk = Reduce(rk_send, rk_recv, rk_s, rk_r, own_dk, sent_dk)
    rv = Reduce(rv_send, rv_recv, rv_s, rv_r, own_dv, sent_dv)

    def hand_out(base, low, high, partial, reduce):
        first = base // tok
        reduce.hand(first + low, first + high, "start")

        def keep(block, out):
            at = pl.ds(pl.multiple_of((block - first) * tok, tok), tok)
            out[...] = partial[at, :]

        if spans == 1:
            if high == per_span:
                keep(s, reduce.own)
                if half:
                    pl.when(s >= half)(lambda: keep(s - half, reduce.sent))
        else:
            for block, out in ((s, reduce.own), (s - half, reduce.sent)):
                @pl.when(jnp.logical_and(block >= first + low, block < first + high))
                def _(block=block, out=out):
                    keep(block, out)

    def store_parts(base, c, value, partial, send):
        partial[c * chunk:(c + 1) * chunk, :] = value
        for i in range(chunk // tok):
            send[base // tok + c * (chunk // tok) + i] = value[i * tok:(i + 1) * tok].astype(BF16)

    def value_part(base):
        for c in range(span // chunk):
            p = s_scr[at_chunk(base, c), :] * inverse
            s_scr[at_chunk(base, c), :] = p
            low = p.astype(BF16)
            p_scr[at_chunk(base, c), :] = low
            store_parts(base, c, dot_nn(low, g_st[...]), dvp, rv_send)
        hand_out(base, 0, per_span, dvp, rv)

    each_span(value_part)
    v_gather.finish()
    if exchange:
        loop(s + 1, inner * (z + 1), lambda b: x_copy(b).start())

    def weighted(base):
        o_acc[...] += dot_tn(v_all[pl.ds(base, span), :], p_scr[pl.ds(base, span), :])

    each_span(weighted)
    delta = jnp.sum(g_tr[...] * o_acc[...], axis=0, keepdims=True)

    def key_part(base):
        halves = 2 if (span // chunk) % 2 == 0 else 1
        count = span // chunk // halves
        for part_of in range(halves):
            for c in range(part_of * count, (part_of + 1) * count):
                dp = dot_nt(v_all[at_chunk(base, c), :], g_st[...])
                ds = (s_scr[at_chunk(base, c), :] * (dp - delta)).astype(BF16)
                ds_scr[c * chunk:(c + 1) * chunk, :] = ds
                store_parts(base, c, dot_nn(ds, q_st[...]), dkp, rk_send)
            hand_out(base, part_of * per_span // halves, (part_of + 1) * per_span // halves, dkp, rk)
        dq_acc[...] += dot_tn(k_all[pl.ds(base, span), :], ds_scr[...])

    each_span(key_part)
    if hosted:
        wv_gather.held(0, "start")
    for g in range(group):
        at = slice(g * tok, (g + 1) * tok)
        ao_ref[:, g * HD:(g + 1) * HD] = o_acc[:, at].T.astype(BF16)
        gq_ref[:, g * HD:(g + 1) * HD] = (dq_acc[:, at] * scale).T.astype(BF16)


    if exchange:
        loop(0, s, x_arrived)
        loop(s + 1, n, x_arrived)
        loop(1, nf, lambda d: xf_copy(d).start())
    def drain_early():
        move_weights("wait_send")
        relay_weights("wait_send", 1, outer)
        if hosted:
            for way in (0, 1):
                wv_gather.held(way, "wait_send")
            guests.drain()
        if exchange:
            loop(0, s, lambda b: x_copy(b).wait_send())
            loop(s + 1, n, lambda b: x_copy(b).wait_send())

    for gather in (k_gather, v_gather):
        gather.drain()
    rv.pass_on()
    rk.pass_on()
    @pl.when(z < outer // 2)
    def _():
        if hosted:
            pl.when(z == 0)(lambda: last_relays("start", (wv_gather,)))
        drain_early()

    if hosted:
        pl.when(z > outer // 2)(lambda: pl.semaphore_wait(told.at[0], 1))
        pl.when(jnp.logical_and(z >= outer // 2, z < last))(lambda: tell(0, s + inner))
    rv.take()
    dv_all[own_rows, :] = own_dv[...].astype(BF16)
    dv_gather.start()
    rk.take()
    lin = own_dk[...] * scale
    turned = lin * cos_scr[...] - pltpu.roll(lin, HD // 2, 1) * sin_scr[...]
    dk_all[own_rows, :] = turned.astype(BF16)
    dk_gather.start()

    def input_term(b):
        at = pl.ds(pl.multiple_of(b * width, width), width)
        return (dot_nt(dk_all[own_rows, :], wk_all[at, :])
                + dot_nt(dv_all[own_rows, :], wv_all[at, :]))

    def gi_twin(o):
        return copy(gi_send.at[o], gi_recv.at[o], gi_s.at[o], gi_r.at[o], (s, twin))

    def gi_far(d):
        return copy(gi_send.at[chips + d], gi_recv.at[chips + chip], gi_s.at[chips + d],
                    gi_r.at[chips + chip], (s, (chip + d) % chips * cores + core))

    def twin_term(d):
        o = (chip + d) % chips
        gi_send[o] = input_term(o * cores + 1 - core).astype(BF16)
        gi_twin(o).start()

    def own_term(d):
        o = (chip + d) % chips
        gi_own[o] = input_term(o * cores + core)

    def join(d):
        o = (chip + d) % chips
        gi_twin(o).wait_recv()
        gi_own[o] += gi_recv[o].astype(F32)

    def far_term(d):
        if cores == 2:
            join(d)
        gi_send[chips + d] = gi_own[(chip + d) % chips].astype(BF16)
        gi_far(d).start()

    def far_terms(d):
        if cores == 2:
            twin_term(d)
        own_term(d)
        far_term(d)

    if hosted:
        pl.when(z == last)(lambda: last_relays("start", (wv_gather,)))

        @pl.when(is_end(z))
        def _():
            for gather in (wk_gather, wv_gather):
                gather.finish(last - z, last - z + 1)

    loop(1, chips, far_terms)
    if cores == 2:
        twin_term(0)
    own_term(0)

    def weight_grad(grads, out):
        if exchange:
            out[...] = dot_tn(grads[...], x_all[...]).T
        else:
            grad = None
            step = min(total, 1024)
            for at in range(0, total, step):
                term = dot_tn(xt_in[at:at + step, :], grads[at:at + step, :])
                grad = term if grad is None else grad + term
            out[...] = grad

    pl.when(z >= outer // 2)(drain_early)
    dv_gather.forward()
    dk_gather.forward()
    dv_gather.finish()
    if exchange:
        loop(1, nf, xf_arrived)
    weight_grad(dv_all, gwv_ref)
    dk_gather.finish()
    weight_grad(dk_all, gwk_ref)

    def gi_take(d):
        b = (chip + d) % chips
        copy(gi_send.at[chips + d], gi_recv.at[chips + b], gi_s.at[chips + d],
             gi_r.at[chips + b], (s, b * cores + core)).wait_recv()
        gi_own[chip] += gi_recv[chips + b].astype(F32)

    if cores == 2:
        join(0)
    loop(1, chips, gi_take)
    gi_ref[...] = gi_own[chip].astype(BF16)

    for gather in (dk_gather, dv_gather):
        gather.drain()
    if exchange:
        loop(1, nf, lambda d: xf_copy(d).wait_send())
    rv.drain()
    rk.drain()
    if cores == 2:
        loop(0, chips, lambda o: gi_twin(o).wait_send())
    loop(1, chips, lambda d: gi_far(d).wait_send())


def publish(*refs):
    count = len(refs) // 2
    sems = refs[-1]
    moves = [pltpu.make_async_copy(refs[i], refs[count + i], sems.at[i]) for i in range(count)]
    for move in moves:
        move.start()
    for move in moves:
        move.wait()


def body(n, nf, queries, layer_input, w_key, w_value, grad_out):
    tok, depth = layer_input.shape
    rows, cols = w_key.shape
    assert cols == HD
    group = queries.shape[1] // cols
    m_cols = group * tok
    part = rows // nf
    exchange = part % 128 == 0
    half = HD // 2
    freq = np.float32(ROPE_BASE) ** (-(np.arange(half, dtype=np.float32) * np.float32(2.0 / HD)))
    freq = jnp.asarray(np.concatenate([freq, freq])[None, :], F32)
    operands = [queries, layer_input, w_key, w_value, grad_out, freq]
    if not exchange:
        operands.append(
            lax.all_to_all(layer_input, "seq", split_axis=1, concat_axis=0, tiled=True))
    width = depth // nf
    total = n * tok
    span = math.gcd(total, 1024)
    inner = 2 if n % 2 == 0 else 1
    outer = n // inner
    pieces = len(pieces_of(rows, inner))
    hops = 3 * outer + (2 * n + outer if pieces > 1 else 0)
    vmem = pltpu.VMEM
    dma = pltpu.SemaphoreType.DMA
    scratch = [vmem((depth, cols), BF16)] * 2
    scratch += [vmem((total, cols), BF16)] * 4
    scratch += [
        vmem((total, rows) if exchange else (16, 128), BF16),
        vmem((m_cols, HD), BF16), vmem((m_cols, HD), BF16), vmem((HD, m_cols), F32),
        vmem((total, m_cols), F32), vmem((total, m_cols), BF16), vmem((span, m_cols), BF16),
        vmem((8, m_cols), F32), vmem((8, m_cols), F32),
        vmem((HD, m_cols), F32), vmem((HD, m_cols), F32),
        vmem((span, cols), F32), vmem((span, cols), F32),
    ]
    slots = n + n // 2
    scratch += [vmem((n, tok, cols), BF16), vmem((slots, tok, cols), BF16)] * 2
    scratch += [vmem((tok, cols), F32)] * 6
    scratch += [
        vmem((2 * nf, tok, width), BF16), vmem((2 * nf, tok, width), BF16),
        vmem((nf, tok, width), F32),
    ]
    scratch += [vmem((tok, inner * rows), BF16)]
    scratch += [vmem((2, tok, cols), BF16)] * 2
    scratch += [pltpu.SemaphoreType.REGULAR((2,))]
    scratch += [dma((2 * nf,)), dma((nf,)), dma((2,)), dma((2,))]
    scratch += [dma((hops,)), dma((pieces * n,))] * 2
    scratch += [dma((2 * outer + 1,)), dma((n,))] * 2
    scratch += [dma((1,)), dma((1,))] * 2 if exchange else [dma((2 * outer + 1,)), dma((n,))] * 2
    scratch += [dma((n,)), dma((n,)), dma((nf,)), dma((nf,))]
    scratch += [dma((n,)), dma((slots,))] * 2
    scratch += [dma((2 * nf,)), dma((2 * nf,))]
    scratch += [vmem(queries.shape, BF16), vmem((tok, depth), BF16), vmem(queries.shape, BF16),
                dma((5,))]
    out_shape = [
        jax.ShapeDtypeStruct(queries.shape, BF16),
        jax.ShapeDtypeStruct(queries.shape, BF16),
        jax.ShapeDtypeStruct((tok, width), BF16),
        jax.ShapeDtypeStruct((rows, cols), F32),
        jax.ShapeDtypeStruct((rows, cols), F32),
    ]
    spec = pl.BlockSpec(memory_space=pltpu.VMEM)
    whole = pl.BlockSpec(memory_space=pl.ANY)
    results = pl.pallas_call(
        functools.partial(kernel, (n, nf, exchange)),
        out_shape=[pltpu.VMEM(o.shape, o.dtype) for o in out_shape],
        in_specs=[whole] * 5 + [spec] * (len(operands) - 5),
        out_specs=[spec] * len(out_shape),
        scratch_shapes=scratch,
        compiler_params=pltpu.CompilerParams(
            collective_id=0, has_side_effects=True, vmem_limit_bytes=60 * 1024 * 1024),
    )(*operands)
    return tuple(pl.pallas_call(
        publish,
        out_shape=out_shape,
        in_specs=[spec] * len(out_shape),
        out_specs=[whole] * len(out_shape),
        scratch_shapes=[dma((len(out_shape),))],
        compiler_params=pltpu.CompilerParams(vmem_limit_bytes=8 * 1024 * 1024),
    )(*results))


def solution(mesh):
    placed = (
        P("seq", "fsdp"),
        P("seq", None),
        P("seq", "fsdp"),
        P("seq", "fsdp"),
        P("seq", "fsdp"),
    )
    return jax.shard_map(
        functools.partial(body, mesh.shape["seq"], mesh.shape["fsdp"]),
        mesh=mesh,
        in_specs=placed,
        out_specs=(P("seq", "fsdp"),) * 5,
        check_vma=False,
    )
```

```python
import functools
import math

import jax
import jax.numpy as jnp
import numpy as np
from jax import lax
from jax.experimental import pallas as pl
from jax.experimental.pallas import tpu as pltpu
from jax.sharding import PartitionSpec as P

HD = 128
ROPE_BASE = 500000.0
NEG = -1e30
MESH = pl.DeviceIdType.MESH
F32 = jnp.float32
BF16 = jnp.bfloat16


def loop(low, high, step):
    def run(i, carry):
        step(i)
        return carry

    lax.fori_loop(low, high, run, 0)


def dot_nn(a, b):
    return lax.dot_general(a, b, (((1,), (0,)), ((), ())), preferred_element_type=F32)


def dot_nt(a, b):
    return lax.dot_general(a, b, (((1,), (1,)), ((), ())), preferred_element_type=F32)


def dot_tn(a, b):
    return lax.dot_general(a, b, (((0,), (0,)), ((), ())), preferred_element_type=F32)


def block_of(ref, b, size):
    return ref.at[pl.ds(pl.multiple_of(b * size, size), size)]


def pieces_of(rows, inner):
    late = rows * 5 // 8 // 16 * 16 if inner == 2 else 0
    return [(0, rows - late, False)] + ([(rows - late, late, True)] if late else [])


def kernel(cfg, *refs):
    n, nf, exchange = cfg
    q_hbm, x_hbm, wk_ref, wv_ref, g_hbm, freq_ref = refs[:6]
    refs = refs[6:]
    if not exchange:
        xt_in = refs[0]
        refs = refs[1:]
    ao_ref, gq_ref, gi_ref, gwk_ref, gwv_ref = refs[:5]
    (wk_all, wv_all, k_all, v_all, dk_all, dv_all, x_all, q_st, g_st, g_tr,
     s_scr, p_scr, ds_scr, m_scr, l_scr, o_acc, dq_acc, dkp, dvp,
     rk_send, rk_recv, rv_send, rv_recv, own_dk, own_dv, sent_dk, sent_dv, cos_scr, sin_scr,
     gi_send, gi_recv, gi_own, xg, pe_send, pe_recv,
     told, xe_s, xe_r, pe_s, pe_r, wk_s, wk_r, wv_s, wv_r, k_s, k_r, v_s, v_r, dk_s, dk_r, dv_s, dv_r,
     x_s, x_r, xf_s, xf_r, rk_s, rk_r, rv_s, rv_r, gi_s, gi_r,
     q_ref, x_ref, g_ref, in_s) = refs[5:]
    tok = x_ref.shape[0]
    rows, cols = wk_ref.shape
    group = q_ref.shape[1] // cols
    m_cols = group * tok
    part = rows // nf
    width = gi_ref.shape[1]
    total = n * tok
    span = ds_scr.shape[0]
    spans = total // span
    per_span = span // tok
    chunk = math.gcd(span, 256)
    scale = HD ** (-0.5)
    s = lax.axis_index("seq")
    f = lax.axis_index("fsdp")
    inner = 2 if n % 2 == 0 else 1
    outer = n // inner
    z = s // inner
    y = s % inner
    mate = z * inner + (inner - 1 - y)
    last = outer - 1
    hosted = exchange and inner == 2 and outer >= 4
    cores = 2 if nf % 2 == 0 else 1
    chips = nf // cores
    chip = f // cores
    core = f % cores
    twin = chip * cores + (cores - 1 - core)

    def copy(src, dst, send, recv, dev):
        return pltpu.make_async_remote_copy(
            src_ref=src, dst_ref=dst, send_sem=send, recv_sem=recv, device_id=dev,
            device_id_type=MESH,
        )

    barrier = pltpu.get_barrier_semaphore()

    def greet(b):
        pl.semaphore_signal(barrier, inc=1, device_id=(b, f), device_id_type=MESH)

    def greet_fsdp(d):
        pl.semaphore_signal(
            barrier, inc=1, device_id=(s, (f + d) % nf), device_id_type=MESH)

    pl.when(z < outer - 1)(lambda: greet(s + inner))
    pl.when(z > 0)(lambda: greet(s - inner))
    if inner == 2:
        greet(mate)
    loop(1, nf, greet_fsdp)
    loads = [
        pltpu.make_async_copy(src, dst, in_s.at[i])
        for i, (src, dst) in enumerate((
            (wk_ref, block_of(wk_all, s, rows)), (wv_ref, block_of(wv_all, s, rows)),
            (x_hbm, x_ref), (q_hbm, q_ref), (g_hbm, g_ref)))
    ]
    for load in loads:
        load.start()

    def clear(b):
        at = pl.ds(pl.multiple_of(b * tok, tok), tok)
        k_all[at, :] = jnp.zeros((tok, cols), BF16)
        v_all[at, :] = jnp.zeros((tok, cols), BF16)

    loop(inner * (z + 1), n, clear)
    pl.semaphore_wait(
        barrier, jnp.minimum(z, 1) + jnp.minimum(outer - 1 - z, 1) + nf + inner - 2)

    class Gather:
        def __init__(self, ref, send, recv, causal=False):
            self.slot = lambda b: block_of(ref, b, tok)
            self.send, self.recv, self.causal = send, recv, causal

        def move(self, b, sem, level, row):
            ref = self.slot(b)
            return copy(ref, ref, self.send.at[sem], self.recv.at[b], (level * inner + row, f))

        def arrived(self, b):
            self.move(b, 0, z, y).wait_recv()

        def ends(self):
            return z == 0 if self.causal else jnp.logical_or(z == 0, z == outer - 1)

        def sends(self, act):
            def run(sem, level, row):
                getattr(self.move(s, sem, level, row), act)()

            def near(d):
                pl.when(z + d < outer)(lambda: run(z + d, z + d, y))
                if not self.causal:
                    pl.when(z >= d)(lambda: run(z - d, z - d, y))

            def far():
                if inner == 2 and outer > 1:
                    pl.when(self.ends())(lambda: run(z, outer - 1 - z, 1 - y))

            def to_mate():
                if inner == 2:
                    run(outer, z, 1 - y)

            if self.causal:
                far()
                loop(0, outer - 1, lambda i: near(outer - 1 - i))
                to_mate()
            else:
                to_mate()
                loop(1, outer, near)
                far()

        def start(self):
            self.sends("start")

        def relay(self, act, low=1, high=outer):
            def step(d):
                def pass_on(level):
                    b = level * inner + y
                    if act == "start":
                        self.arrived(b)
                    if inner == 2:
                        far = jnp.logical_or(level - z == outer - 1, z - level == outer - 1)
                        pl.when(jnp.logical_not(far))(lambda: getattr(
                            self.move(b, outer + 1 + level, z, 1 - y), act)())

                pl.when(z >= d)(lambda: pass_on(z - d))
                if not self.causal:
                    pl.when(z + d < outer)(lambda: pass_on(z + d))

            loop(low, high, step)

        def forward(self, low=1, high=outer):
            self.relay("start", low, high)

        def finish(self):
            if inner == 2:
                loop(0, z + 1 if self.causal else outer,
                     lambda level: self.arrived(level * inner + 1 - y))

        def drain(self):
            self.sends("wait_send")
            self.relay("wait_send")

    pieces = pieces_of(rows, inner)

    def is_end(level):
        return jnp.logical_or(level == 0, level == outer - 1)

    class Weights:
        def __init__(self, ref, send, recv, deferred=False):
            self.ref, self.send, self.recv, self.deferred = ref, send, recv, deferred

        def hop(self, q, b, way):
            at, count, late = pieces[q]
            ref = self.ref.at[pl.ds(pl.multiple_of(b * rows + at, 16), count)]
            dev = ((z + 1) * inner + y, (z - 1) * inner + y, mate)[way]
            if late:
                sem = 3 * outer + (2 * n + b // inner if way == 2 else way * n + b)
            else:
                sem = way * outer + b // inner
            return copy(ref, ref, self.send.at[sem], self.recv.at[q * n + b], (dev, f))

        def arrived(self, q, b):
            self.hop(q, b, 2).wait_recv()

        def own(self, q, way, act):
            def go():
                getattr(self.hop(q, s, way), act)()

            if way == 0:
                pl.when(z < outer - 1)(go)
            elif way == 1:
                pl.when(z > 0)(go)
            elif inner == 2:
                go()

        def mates(self, act):
            for q, (_, _, late) in enumerate(pieces):
                if late:
                    @pl.when(is_end(z))
                    def _(q=q):
                        if act == "start":
                            self.arrived(q, mate)
                        pl.when(z < outer - 1)(lambda: getattr(self.hop(q, mate, 0), act)())
                        pl.when(z > 0)(lambda: getattr(self.hop(q, mate, 1), act)())

        def relay(self, q, d, act):
            late = pieces[q][2]

            def one(b, way, to_mate):
                more = z < last if way == 0 else z > 0
                if self.deferred:
                    more = jnp.logical_and(more, jnp.logical_not(
                        jnp.logical_and(z == last - 1, b // inner == 0) if way == 0
                        else jnp.logical_and(z == 1, b // inner == last)))
                if act == "start":
                    self.arrived(q, b)
                pl.when(more)(lambda: getattr(self.hop(q, b, way), act)())
                if to_mate:
                    getattr(self.hop(q, b, 2), act)()

            def pass_on(level, way):
                if late:
                    end = is_end(level)

                    @pl.when(end)
                    def _():
                        for line in range(inner):
                            one(level * inner + line, way, False)

                    pl.when(jnp.logical_not(end))(lambda: one(level * inner + y, way, True))
                else:
                    one(level * inner + y, way, inner == 2)

            pl.when(z >= d)(lambda: pass_on(z - d, 0))
            pl.when(z + d < outer)(lambda: pass_on(z + d, 1))

        def held(self, way, act):
            def run():
                for q, (_, _, late) in enumerate(pieces):
                    for line in range(inner) if late else (y,):
                        level = last if way == 1 else 0
                        getattr(self.hop(q, level * inner + line, way), act)()

            pl.when(z == (1 if way == 1 else last - 1))(run)

        def finish(self, low=0, high=outer):
            if inner == 2:
                def step(level):
                    for q, (_, _, late) in enumerate(pieces):
                        def go(q=q):
                            self.arrived(q, level * inner + (1 - y))

                        if late:
                            pl.when(jnp.logical_not(is_end(level)))(go)
                        else:
                            go()

                loop(low, high, step)

    def move_weights(act):
        for gather in (wk_gather, wv_gather):
            for q in range(len(pieces)):
                gather.own(q, 0, act)
                gather.own(q, 1, act)
            for q in range(len(pieces) - 1, -1, -1):
                gather.own(q, 2, act)
            gather.mates(act)

    def relay_weights(act, low, high):
        def step(d):
            for gather in (wk_gather, wv_gather):
                for q in range(len(pieces)):
                    gather.relay(q, d, act)

        loop(low, high, step)

    def when_host(act):
        pl.when(jnp.logical_or(z == 1, z == last - 1))(act)

    class Guest:
        def __init__(self):
            self.span = inner * rows
            self.part = self.span // nf

        def place(self, p):
            return xg.at[:, pl.ds(pl.multiple_of(p * self.part, 128), self.part)]

        def move(self, p, sem, dev):
            return copy(self.place(p), self.place(p), xe_s.at[sem], xe_r.at[p], dev)

        def arrived(self, p):
            self.move(p, 0, (s, f)).wait_recv()

        def leave(self, act):
            @pl.when(is_end(z))
            def _():
                host = jnp.minimum(jnp.maximum(z, 1), last - 1) * inner + y
                at = pl.multiple_of((last - z) * self.span + f * self.part, 128)
                getattr(copy(x_ref.at[:, pl.ds(at, self.part)], self.place(f), xe_s.at[0],
                             xe_r.at[f], (host, f)), act)()

        def spread(self, act):
            def run():
                if act == "start":
                    self.arrived(f)
                loop(1, chips, lambda d: getattr(self.move(
                    f, d, (s, (chip + d) % chips * cores + core)), act)())
                if cores == 2:
                    getattr(self.move(f, chips + chip, (s, twin)), act)()

            when_host(run)

        def share(self, act):
            def step(d):
                o = (chip + d) % chips
                if act == "start":
                    self.arrived(o * cores + core)
                if cores == 2:
                    getattr(self.move(o * cores + core, chips + o, (s, twin)), act)()

            when_host(lambda: loop(1, chips, step))

        def finish(self):
            if cores == 2:
                loop(0, chips, lambda o: self.arrived(o * cores + 1 - core))

        def reply(self, i):
            end = jnp.minimum(z - 1, 1) * last
            return copy(pe_send.at[i], pe_recv.at[i], pe_s.at[i], pe_r.at[i], (end * inner + y, f))

        def partial(self, i, weights):
            def run():
                at = (last - jnp.minimum(z - 1, 1) * last) * self.span
                w = weights[pl.ds(pl.multiple_of(at, 16), self.span), :]
                pe_send[i] = dot_nn(xg[...], w).astype(BF16)
                self.reply(i).start()

            when_host(run)

        def rest(self, weights):
            at = pl.multiple_of(z // last * self.span, 128)
            here = pl.ds(at, (outer - 1) * self.span)
            return dot_nn(x_ref[:, here], weights[here, :])

        def returned(self, i):
            copy(pe_send.at[i], pe_recv.at[i], pe_s.at[i], pe_r.at[i], (mate, f)).wait_recv()
            return pe_recv[i].astype(F32)

        def drain(self):
            self.leave("wait_send")
            self.spread("wait_send")
            self.share("wait_send")
            when_host(lambda: loop(0, 2, lambda i: self.reply(i).wait_send()))

    wk_gather = Weights(wk_all, wk_s, wk_r)
    wv_gather = Weights(wv_all, wv_s, wv_r, deferred=hosted)
    guests = Guest() if hosted else None
    k_gather = Gather(k_all, k_s, k_r, causal=True)
    v_gather = Gather(v_all, v_s, v_r, causal=True)
    dk_gather = Gather(dk_all, *((v_s, v_r) if exchange else (dk_s, dk_r)))
    dv_gather = Gather(dv_all, *((k_s, k_r) if exchange else (dv_s, dv_r)))

    for load in loads[:3]:
        load.wait()
    if hosted:
        guests.leave("start")
    move_weights("start")
    for load in loads[3:]:
        load.wait()

    own_rows = pl.ds(pl.multiple_of(s * tok, tok), tok)
    if exchange:
        own_part = pl.ds(pl.multiple_of(f * part, 128), part)

        def x_src(b):
            return x_ref.at[:, pl.ds(pl.multiple_of(b * rows + f * part, 128), part)]

        def x_slot(b, at):
            return x_all.at[pl.ds(pl.multiple_of(b * tok, tok), tok), at]

        def x_copy(b):
            return copy(x_src(b), x_slot(s, own_part), x_s.at[b], x_r.at[s], (b, f))

        def x_arrived(b):
            copy(x_src(b), x_slot(b, own_part), x_s.at[b], x_r.at[b], (b, f)).wait_recv()

        def xf_copy(d):
            ref = x_all.at[:, own_part]
            return copy(ref, ref, xf_s.at[d], xf_r.at[f], (s, (f + d) % nf))

        def xf_arrived(d):
            b = (f + d) % nf
            ref = x_all.at[:, pl.ds(pl.multiple_of(b * part, 128), part)]
            copy(ref, ref, xf_s.at[d], xf_r.at[b], (s, b)).wait_recv()

        x_all[own_rows, own_part] = x_ref[
            :, pl.ds(pl.multiple_of(s * rows + f * part, 128), part)]

    for g in range(group):
        at = slice(g * tok, (g + 1) * tok)
        q_st[at, :] = q_ref[:, g * HD:(g + 1) * HD]
        up = g_ref[:, g * HD:(g + 1) * HD]
        g_st[at, :] = up
        g_tr[:, at] = up.astype(F32).T
    lane = lax.broadcasted_iota(jnp.int32, (tok, HD), 1)
    position = (s * tok + lax.broadcasted_iota(jnp.int32, (tok, HD), 0)).astype(F32)
    angle = position * freq_ref[...]
    cos_scr[...] = jnp.cos(angle)
    sin_scr[...] = jnp.where(lane < HD // 2, -jnp.sin(angle), jnp.sin(angle))

    def tell(which, device):
        pl.semaphore_signal(
            told.at[which], inc=1, device_id=(device, f), device_id_type=MESH)

    if hosted:
        pl.when(z < last - 1)(lambda: pl.semaphore_wait(told.at[0], 1))
        pl.when(jnp.logical_and(z > 0, z < last))(lambda: tell(0, s - inner))

        @pl.when(z == 0)
        def _():
            tell(1, mate)
            pl.semaphore_wait(told.at[1], 1)

    relay_weights("start", 1, 2)
    if hosted:
        guests.spread("start")
    relay_weights("start", 2, outer - 1)
    if hosted:
        guests.share("start")
    def x_ahead():
        loop(inner * (z + 1), n, lambda b: x_copy(b).start())

    if hosted:
        pl.when(z == 0)(x_ahead)

    def last_relays(act, gathers):
        for gather in gathers:
            for q in range(len(pieces)):
                gather.relay(q, outer - 1, act)

    def rotated(lin):
        return lin * cos_scr[...] + pltpu.roll(lin, HD // 2, 1) * sin_scr[...]

    def finish_levels(low, high):
        wk_gather.finish(low, high)
        wv_gather.finish(low, high)

    def keep_keys(lin):
        k_all[own_rows, :] = rotated(lin).astype(BF16)
        k_gather.start()

    def keep_values(value):
        v_all[own_rows, :] = value.astype(BF16)
        v_gather.start()

    def project():
        keep_keys(dot_nn(x_ref[...], wk_all[...]))
        keep_values(dot_nn(x_ref[...], wv_all[...]))

    def project_end():
        first = jnp.minimum(z, 1)
        with jax.named_scope("wkfin"):
            finish_levels(first, first + outer - 1)
        with jax.named_scope("kproj"):
            keys, values = guests.rest(wk_all), guests.rest(wv_all)
        with jax.named_scope("xfin"):
            keep_keys(keys + guests.returned(0))
        with jax.named_scope("vproj"):
            keep_values(values + guests.returned(1))

    def project_inner():
        with jax.named_scope("wkfin"):
            finish_levels(0, outer)
        with jax.named_scope("xfin"):
            pl.when(z < last - 1)(x_ahead)
            when_host(guests.finish)
        with jax.named_scope("kproj"):
            guests.partial(0, wk_all)
            guests.partial(1, wv_all)
        with jax.named_scope("vproj"):
            project()

    if hosted:
        pl.when(is_end(z))(project_end)
        pl.when(jnp.logical_not(is_end(z)))(project_inner)
    else:
        if outer > 1:
            last_relays("start", (wk_gather, wv_gather))
        finish_levels(0, outer)
        project()
    if hosted:
        wv_gather.held(1, "start")
    if exchange:
        pl.when(z == last - 1)(x_ahead) if hosted else x_ahead()
        loop(0, s, lambda b: x_copy(b).start())
    k_gather.forward()
    v_gather.forward()
    if hosted:
        last_relays("start", (wk_gather,))
    k_gather.finish()
    def each_span(step):
        if spans == 1:
            step(0)
        else:
            loop(0, s * tok // span + 1, lambda i: step(pl.multiple_of(i * span, span)))

    def at_chunk(base, c):
        return pl.ds(base + c * chunk, chunk)

    def fold(value):
        return value.reshape(chunk // 8, 8, m_cols)

    column = jnp.concatenate(
        [lax.broadcasted_iota(jnp.int32, (chunk, tok), 1)] * group, axis=1)
    ahead = lax.broadcasted_iota(jnp.int32, (chunk, m_cols), 0) - column

    m_scr[...] = jnp.full(m_scr.shape, NEG, F32)
    l_scr[...] = jnp.zeros(l_scr.shape, F32)
    o_acc[...] = jnp.zeros(o_acc.shape, F32)
    dq_acc[...] = jnp.zeros(dq_acc.shape, F32)

    def score(base):
        for c in range(span // chunk):
            sc = dot_nt(k_all[at_chunk(base, c), :], q_st[...])
            sc = jnp.where(ahead <= s * tok - base - c * chunk, sc, NEG)
            s_scr[at_chunk(base, c), :] = sc
            m_scr[...] = jnp.maximum(m_scr[...], jnp.max(fold(sc), axis=0))

    each_span(score)
    top = jnp.max(m_scr[...], axis=0, keepdims=True)

    def weigh(base):
        for c in range(span // chunk):
            e = jnp.exp2((s_scr[at_chunk(base, c), :] - top) * (scale * math.log2(math.e)))
            s_scr[at_chunk(base, c), :] = e
            l_scr[...] += jnp.sum(fold(e), axis=0)

    each_span(weigh)
    inverse = 1.0 / jnp.sum(l_scr[...], axis=0, keepdims=True)

    half = n // 2 if n % 2 == 0 else 0
    low_end = s // half * half if half else 0

    class Reduce:
        def __init__(self, send, recv, send_sem, recv_sem, own, sent):
            self.send, self.recv, self.send_sem, self.recv_sem = send, recv, send_sem, recv_sem
            self.own, self.sent = own, sent

        def direct(self, j):
            return copy(self.send.at[j], self.recv.at[s], self.send_sem.at[j], self.recv_sem.at[s],
                        (j, f))

        def inward(self, j):
            slot = n + s - half
            return copy(self.send.at[j], self.recv.at[slot], self.send_sem.at[j],
                        self.recv_sem.at[slot], (j + half, f))

        def got(self, slot):
            copy(self.send.at[0], self.recv.at[slot], self.send_sem.at[0], self.recv_sem.at[slot],
                 (mate, f)).wait_recv()
            return self.recv[slot].astype(F32)

        def hand(self, low, high, act):
            high = jnp.minimum(high, s)
            loop(jnp.maximum(low, low_end), high, lambda j: getattr(self.direct(j), act)())
            if half:
                @pl.when(s >= half)
                def _():
                    loop(low, jnp.minimum(high, half), lambda j: pl.when(j + half != s)(
                        lambda: getattr(self.inward(j), act)()))

        def pass_on(self):
            if half:
                @pl.when(s >= half)
                def _():
                    def add(i):
                        self.sent[...] += self.got(n + i - half)

                    loop(half, s, add)
                    loop(s + 1, n, add)
                    self.send[s - half] = self.sent[...].astype(BF16)
                    self.direct(s - half).start()

        def take(self):
            def add(j):
                self.own[...] += self.got(j)

            loop(s + 1, low_end + half if half else n, add)
            if half:
                pl.when(s < half)(lambda: add(s + half))

        def drain(self):
            self.hand(0, n, "wait_send")
            if half:
                pl.when(s >= half)(lambda: self.direct(s - half).wait_send())

    rk = Reduce(rk_send, rk_recv, rk_s, rk_r, own_dk, sent_dk)
    rv = Reduce(rv_send, rv_recv, rv_s, rv_r, own_dv, sent_dv)

    def hand_out(base, low, high, partial, reduce):
        first = base // tok
        reduce.hand(first + low, first + high, "start")

        def keep(block, out):
            at = pl.ds(pl.multiple_of((block - first) * tok, tok), tok)
            out[...] = partial[at, :]

        if spans == 1:
            if high == per_span:
                keep(s, reduce.own)
                if half:
                    pl.when(s >= half)(lambda: keep(s - half, reduce.sent))
        else:
            for block, out in ((s, reduce.own), (s - half, reduce.sent)):
                @pl.when(jnp.logical_and(block >= first + low, block < first + high))
                def _(block=block, out=out):
                    keep(block, out)

    def store_parts(base, c, value, partial, send):
        partial[c * chunk:(c + 1) * chunk, :] = value
        for i in range(chunk // tok):
            send[base // tok + c * (chunk // tok) + i] = value[i * tok:(i + 1) * tok].astype(BF16)

    def value_part(base):
        for c in range(span // chunk):
            p = s_scr[at_chunk(base, c), :] * inverse
            s_scr[at_chunk(base, c), :] = p
            low = p.astype(BF16)
            p_scr[at_chunk(base, c), :] = low
            store_parts(base, c, dot_nn(low, g_st[...]), dvp, rv_send)
        hand_out(base, 0, per_span, dvp, rv)

    each_span(value_part)
    v_gather.finish()
    if exchange:
        loop(s + 1, inner * (z + 1), lambda b: x_copy(b).start())

    def weighted(base):
        o_acc[...] += dot_tn(v_all[pl.ds(base, span), :], p_scr[pl.ds(base, span), :])

    each_span(weighted)
    delta = jnp.sum(g_tr[...] * o_acc[...], axis=0, keepdims=True)

    def key_part(base):
        halves = 2 if (span // chunk) % 2 == 0 else 1
        count = span // chunk // halves
        for part_of in range(halves):
            for c in range(part_of * count, (part_of + 1) * count):
                dp = dot_nt(v_all[at_chunk(base, c), :], g_st[...])
                ds = (s_scr[at_chunk(base, c), :] * (dp - delta)).astype(BF16)
                ds_scr[c * chunk:(c + 1) * chunk, :] = ds
                store_parts(base, c, dot_nn(ds, q_st[...]), dkp, rk_send)
            hand_out(base, part_of * per_span // halves, (part_of + 1) * per_span // halves, dkp, rk)
        dq_acc[...] += dot_tn(k_all[pl.ds(base, span), :], ds_scr[...])

    each_span(key_part)
    if hosted:
        wv_gather.held(0, "start")
    for g in range(group):
        at = slice(g * tok, (g + 1) * tok)
        ao_ref[:, g * HD:(g + 1) * HD] = o_acc[:, at].T.astype(BF16)
        gq_ref[:, g * HD:(g + 1) * HD] = (dq_acc[:, at] * scale).T.astype(BF16)


    if exchange:
        loop(0, s, x_arrived)
        loop(s + 1, n, x_arrived)
        loop(1, nf, lambda d: xf_copy(d).start())
    def drain_early():
        move_weights("wait_send")
        relay_weights("wait_send", 1, outer)
        if hosted:
            for way in (0, 1):
                wv_gather.held(way, "wait_send")
            guests.drain()
        if exchange:
            loop(0, s, lambda b: x_copy(b).wait_send())
            loop(s + 1, n, lambda b: x_copy(b).wait_send())

    for gather in (k_gather, v_gather):
        gather.drain()
    rv.pass_on()
    rk.pass_on()
    @pl.when(z < outer // 2)
    def _():
        if hosted:
            pl.when(z == 0)(lambda: last_relays("start", (wv_gather,)))
        drain_early()

    if hosted:
        pl.when(z > outer // 2)(lambda: pl.semaphore_wait(told.at[0], 1))

        @pl.when(jnp.logical_and(z >= outer // 2, z < last))
        def _():
            if cores == 2:
                pl.semaphore_signal(
                    told.at[1], inc=1, device_id=(s, twin), device_id_type=MESH)
                pl.semaphore_wait(told.at[1], 1)
            tell(0, s + inner)

    rv.take()
    dv_all[own_rows, :] = own_dv[...].astype(BF16)
    dv_gather.start()
    rk.take()
    lin = own_dk[...] * scale
    turned = lin * cos_scr[...] - pltpu.roll(lin, HD // 2, 1) * sin_scr[...]
    dk_all[own_rows, :] = turned.astype(BF16)
    dk_gather.start()

    def input_term(b):
        at = pl.ds(pl.multiple_of(b * width, width), width)
        return (dot_nt(dk_all[own_rows, :], wk_all[at, :])
                + dot_nt(dv_all[own_rows, :], wv_all[at, :]))

    def gi_twin(o):
        return copy(gi_send.at[o], gi_recv.at[o], gi_s.at[o], gi_r.at[o], (s, twin))

    def gi_far(d):
        return copy(gi_send.at[chips + d], gi_recv.at[chips + chip], gi_s.at[chips + d],
                    gi_r.at[chips + chip], (s, (chip + d) % chips * cores + core))

    def twin_term(d):
        o = (chip + d) % chips
        gi_send[o] = input_term(o * cores + 1 - core).astype(BF16)
        gi_twin(o).start()

    def own_term(d):
        o = (chip + d) % chips
        gi_own[o] = input_term(o * cores + core)

    def join(d):
        o = (chip + d) % chips
        gi_twin(o).wait_recv()
        gi_own[o] += gi_recv[o].astype(F32)

    def far_term(d):
        if cores == 2:
            join(d)
        gi_send[chips + d] = gi_own[(chip + d) % chips].astype(BF16)
        gi_far(d).start()

    def far_terms(d):
        if cores == 2:
            twin_term(d)
        own_term(d)
        far_term(d)

    if hosted:
        pl.when(z == last)(lambda: last_relays("start", (wv_gather,)))

        @pl.when(is_end(z))
        def _():
            for gather in (wk_gather, wv_gather):
                gather.finish(last - z, last - z + 1)

    loop(1, chips, far_terms)
    if cores == 2:
        twin_term(0)
    own_term(0)

    def weight_grad(grads, out):
        if exchange:
            out[...] = dot_tn(grads[...], x_all[...]).T
        else:
            grad = None
            step = min(total, 1024)
            for at in range(0, total, step):
                term = dot_tn(xt_in[at:at + step, :], grads[at:at + step, :])
                grad = term if grad is None else grad + term
            out[...] = grad

    pl.when(z >= outer // 2)(drain_early)
    dv_gather.forward()
    dk_gather.forward()
    dv_gather.finish()
    if exchange:
        loop(1, nf, xf_arrived)
    weight_grad(dv_all, gwv_ref)
    dk_gather.finish()
    weight_grad(dk_all, gwk_ref)

    def gi_take(d):
        b = (chip + d) % chips
        copy(gi_send.at[chips + d], gi_recv.at[chips + b], gi_s.at[chips + d],
             gi_r.at[chips + b], (s, b * cores + core)).wait_recv()
        gi_own[chip] += gi_recv[chips + b].astype(F32)

    if cores == 2:
        join(0)
    loop(1, chips, gi_take)
    gi_ref[...] = gi_own[chip].astype(BF16)

    for gather in (dk_gather, dv_gather):
        gather.drain()
    if exchange:
        loop(1, nf, lambda d: xf_copy(d).wait_send())
    rv.drain()
    rk.drain()
    if cores == 2:
        loop(0, chips, lambda o: gi_twin(o).wait_send())
    loop(1, chips, lambda d: gi_far(d).wait_send())


def publish(*refs):
    count = len(refs) // 2
    sems = refs[-1]
    moves = [pltpu.make_async_copy(refs[i], refs[count + i], sems.at[i]) for i in range(count)]
    for move in moves:
        move.start()
    for move in moves:
        move.wait()


def body(n, nf, queries, layer_input, w_key, w_value, grad_out):
    tok, depth = layer_input.shape
    rows, cols = w_key.shape
    assert cols == HD
    group = queries.shape[1] // cols
    m_cols = group * tok
    part = rows // nf
    exchange = part % 128 == 0
    half = HD // 2
    freq = np.float32(ROPE_BASE) ** (-(np.arange(half, dtype=np.float32) * np.float32(2.0 / HD)))
    freq = jnp.asarray(np.concatenate([freq, freq])[None, :], F32)
    operands = [queries, layer_input, w_key, w_value, grad_out, freq]
    if not exchange:
        operands.append(
            lax.all_to_all(layer_input, "seq", split_axis=1, concat_axis=0, tiled=True))
    width = depth // nf
    total = n * tok
    span = math.gcd(total, 1024)
    inner = 2 if n % 2 == 0 else 1
    outer = n // inner
    pieces = len(pieces_of(rows, inner))
    hops = 3 * outer + (2 * n + outer if pieces > 1 else 0)
    vmem = pltpu.VMEM
    dma = pltpu.SemaphoreType.DMA
    scratch = [vmem((depth, cols), BF16)] * 2
    scratch += [vmem((total, cols), BF16)] * 4
    scratch += [
        vmem((total, rows) if exchange else (16, 128), BF16),
        vmem((m_cols, HD), BF16), vmem((m_cols, HD), BF16), vmem((HD, m_cols), F32),
        vmem((total, m_cols), F32), vmem((total, m_cols), BF16), vmem((span, m_cols), BF16),
        vmem((8, m_cols), F32), vmem((8, m_cols), F32),
        vmem((HD, m_cols), F32), vmem((HD, m_cols), F32),
        vmem((span, cols), F32), vmem((span, cols), F32),
    ]
    slots = n + n // 2
    scratch += [vmem((n, tok, cols), BF16), vmem((slots, tok, cols), BF16)] * 2
    scratch += [vmem((tok, cols), F32)] * 6
    scratch += [
        vmem((2 * nf, tok, width), BF16), vmem((2 * nf, tok, width), BF16),
        vmem((nf, tok, width), F32),
    ]
    scratch += [vmem((tok, inner * rows), BF16)]
    scratch += [vmem((2, tok, cols), BF16)] * 2
    scratch += [pltpu.SemaphoreType.REGULAR((2,))]
    scratch += [dma((2 * nf,)), dma((nf,)), dma((2,)), dma((2,))]
    scratch += [dma((hops,)), dma((pieces * n,))] * 2
    scratch += [dma((2 * outer + 1,)), dma((n,))] * 2
    scratch += [dma((1,)), dma((1,))] * 2 if exchange else [dma((2 * outer + 1,)), dma((n,))] * 2
    scratch += [dma((n,)), dma((n,)), dma((nf,)), dma((nf,))]
    scratch += [dma((n,)), dma((slots,))] * 2
    scratch += [dma((2 * nf,)), dma((2 * nf,))]
    scratch += [vmem(queries.shape, BF16), vmem((tok, depth), BF16), vmem(queries.shape, BF16),
                dma((5,))]
    out_shape = [
        jax.ShapeDtypeStruct(queries.shape, BF16),
        jax.ShapeDtypeStruct(queries.shape, BF16),
        jax.ShapeDtypeStruct((tok, width), BF16),
        jax.ShapeDtypeStruct((rows, cols), F32),
        jax.ShapeDtypeStruct((rows, cols), F32),
    ]
    spec = pl.BlockSpec(memory_space=pltpu.VMEM)
    whole = pl.BlockSpec(memory_space=pl.ANY)
    results = pl.pallas_call(
        functools.partial(kernel, (n, nf, exchange)),
        out_shape=[pltpu.VMEM(o.shape, o.dtype) for o in out_shape],
        in_specs=[whole] * 5 + [spec] * (len(operands) - 5),
        out_specs=[spec] * len(out_shape),
        scratch_shapes=scratch,
        compiler_params=pltpu.CompilerParams(
            collective_id=0, has_side_effects=True, vmem_limit_bytes=60 * 1024 * 1024),
    )(*operands)
    return tuple(pl.pallas_call(
        publish,
        out_shape=out_shape,
        in_specs=[spec] * len(out_shape),
        out_specs=[whole] * len(out_shape),
        scratch_shapes=[dma((len(out_shape),))],
        compiler_params=pltpu.CompilerParams(vmem_limit_bytes=8 * 1024 * 1024),
    )(*results))


def solution(mesh):
    placed = (
        P("seq", "fsdp"),
        P("seq", None),
        P("seq", "fsdp"),
        P("seq", "fsdp"),
        P("seq", "fsdp"),
    )
    return jax.shard_map(
        functools.partial(body, mesh.shape["seq"], mesh.shape["fsdp"]),
        mesh=mesh,
        in_specs=placed,
        out_specs=(P("seq", "fsdp"),) * 5,
        check_vma=False,
    )
```

```python
import functools
import math

import jax
import jax.numpy as jnp
import numpy as np
from jax import lax
from jax.experimental import pallas as pl
from jax.experimental.pallas import tpu as pltpu
from jax.sharding import PartitionSpec as P

HD = 128
ROPE_BASE = 500000.0
NEG = -1e30
MESH = pl.DeviceIdType.MESH
F32 = jnp.float32
BF16 = jnp.bfloat16


def loop(low, high, step):
    def run(i, carry):
        step(i)
        return carry

    lax.fori_loop(low, high, run, 0)


def dot_nn(a, b):
    return lax.dot_general(a, b, (((1,), (0,)), ((), ())), preferred_element_type=F32)


def dot_nt(a, b):
    return lax.dot_general(a, b, (((1,), (1,)), ((), ())), preferred_element_type=F32)


def dot_tn(a, b):
    return lax.dot_general(a, b, (((0,), (0,)), ((), ())), preferred_element_type=F32)


def block_of(ref, b, size):
    return ref.at[pl.ds(pl.multiple_of(b * size, size), size)]


def pieces_of(rows, inner):
    late = rows * 5 // 8 // 16 * 16 if inner == 2 else 0
    return [(0, rows - late, False)] + ([(rows - late, late, True)] if late else [])


def kernel(cfg, *refs):
    n, nf, exchange = cfg
    q_hbm, x_hbm, wk_ref, wv_ref, g_hbm, freq_ref = refs[:6]
    refs = refs[6:]
    if not exchange:
        xt_in = refs[0]
        refs = refs[1:]
    ao_ref, gq_ref, gi_ref, gwk_ref, gwv_ref = refs[:5]
    (wk_all, wv_all, k_all, v_all, dk_all, dv_all, x_all, q_st, g_st, g_tr,
     s_scr, p_scr, ds_scr, m_scr, l_scr, o_acc, dq_acc, dkp, dvp,
     rk_send, rk_recv, rv_send, rv_recv, own_dk, own_dv, sent_dk, sent_dv, cos_scr, sin_scr,
     gi_send, gi_recv, gi_own, xg, pe_send, pe_recv,
     told, xe_s, xe_r, pe_s, pe_r, wk_s, wk_r, wv_s, wv_r, k_s, k_r, v_s, v_r, dk_s, dk_r, dv_s, dv_r,
     x_s, x_r, xf_s, xf_r, rk_s, rk_r, rv_s, rv_r, gi_s, gi_r,
     q_ref, x_ref, g_ref, in_s) = refs[5:]
    tok = x_ref.shape[0]
    rows, cols = wk_ref.shape
    group = q_ref.shape[1] // cols
    m_cols = group * tok
    part = rows // nf
    width = gi_ref.shape[1]
    total = n * tok
    span = ds_scr.shape[0]
    spans = total // span
    per_span = span // tok
    chunk = math.gcd(span, 256)
    scale = HD ** (-0.5)
    s = lax.axis_index("seq")
    f = lax.axis_index("fsdp")
    inner = 2 if n % 2 == 0 else 1
    outer = n // inner
    z = s // inner
    y = s % inner
    mate = z * inner + (inner - 1 - y)
    last = outer - 1
    hosted = exchange and inner == 2 and outer >= 4
    cores = 2 if nf % 2 == 0 else 1
    chips = nf // cores
    chip = f // cores
    core = f % cores
    twin = chip * cores + (cores - 1 - core)

    def copy(src, dst, send, recv, dev):
        return pltpu.make_async_remote_copy(
            src_ref=src, dst_ref=dst, send_sem=send, recv_sem=recv, device_id=dev,
            device_id_type=MESH,
        )

    barrier = pltpu.get_barrier_semaphore()

    def greet(b):
        pl.semaphore_signal(barrier, inc=1, device_id=(b, f), device_id_type=MESH)

    def greet_fsdp(d):
        pl.semaphore_signal(
            barrier, inc=1, device_id=(s, (f + d) % nf), device_id_type=MESH)

    pl.when(z < outer - 1)(lambda: greet(s + inner))
    pl.when(z > 0)(lambda: greet(s - inner))
    if inner == 2:
        greet(mate)
    loop(1, nf, greet_fsdp)
    loads = [
        pltpu.make_async_copy(src, dst, in_s.at[i])
        for i, (src, dst) in enumerate((
            (wk_ref, block_of(wk_all, s, rows)), (wv_ref, block_of(wv_all, s, rows)),
            (x_hbm, x_ref), (q_hbm, q_ref), (g_hbm, g_ref)))
    ]
    for load in loads:
        load.start()

    def clear(b):
        at = pl.ds(pl.multiple_of(b * tok, tok), tok)
        k_all[at, :] = jnp.zeros((tok, cols), BF16)
        v_all[at, :] = jnp.zeros((tok, cols), BF16)

    loop(inner * (z + 1), n, clear)
    pl.semaphore_wait(
        barrier, jnp.minimum(z, 1) + jnp.minimum(outer - 1 - z, 1) + nf + inner - 2)

    class Gather:
        def __init__(self, ref, send, recv, causal=False):
            self.slot = lambda b: block_of(ref, b, tok)
            self.send, self.recv, self.causal = send, recv, causal

        def move(self, b, sem, level, row):
            ref = self.slot(b)
            return copy(ref, ref, self.send.at[sem], self.recv.at[b], (level * inner + row, f))

        def arrived(self, b):
            self.move(b, 0, z, y).wait_recv()

        def ends(self):
            return z == 0 if self.causal else jnp.logical_or(z == 0, z == outer - 1)

        def sends(self, act):
            def run(sem, level, row):
                getattr(self.move(s, sem, level, row), act)()

            def near(d):
                pl.when(z + d < outer)(lambda: run(z + d, z + d, y))
                if not self.causal:
                    pl.when(z >= d)(lambda: run(z - d, z - d, y))

            def far():
                if inner == 2 and outer > 1:
                    pl.when(self.ends())(lambda: run(z, outer - 1 - z, 1 - y))

            def to_mate():
                if inner == 2:
                    run(outer, z, 1 - y)

            far()
            loop(0, outer - 1, lambda i: near(outer - 1 - i))
            to_mate()

        def start(self):
            self.sends("start")

        def relay(self, act, low=1, high=outer):
            def step(d):
                def pass_on(level):
                    b = level * inner + y
                    if act == "start":
                        self.arrived(b)
                    if inner == 2:
                        far = jnp.logical_or(level - z == outer - 1, z - level == outer - 1)
                        pl.when(jnp.logical_not(far))(lambda: getattr(
                            self.move(b, outer + 1 + level, z, 1 - y), act)())

                pl.when(z >= d)(lambda: pass_on(z - d))
                if not self.causal:
                    pl.when(z + d < outer)(lambda: pass_on(z + d))

            loop(low, high, step)

        def forward(self, low=1, high=outer):
            self.relay("start", low, high)

        def finish(self):
            if inner == 2:
                loop(0, z + 1 if self.causal else outer,
                     lambda level: self.arrived(level * inner + 1 - y))

        def drain(self):
            self.sends("wait_send")
            self.relay("wait_send")

    pieces = pieces_of(rows, inner)

    def is_end(level):
        return jnp.logical_or(level == 0, level == outer - 1)

    class Weights:
        def __init__(self, ref, send, recv, deferred=False):
            self.ref, self.send, self.recv, self.deferred = ref, send, recv, deferred

        def hop(self, q, b, way):
            at, count, late = pieces[q]
            ref = self.ref.at[pl.ds(pl.multiple_of(b * rows + at, 16), count)]
            dev = ((z + 1) * inner + y, (z - 1) * inner + y, mate)[way]
            if late:
                sem = 3 * outer + (2 * n + b // inner if way == 2 else way * n + b)
            else:
                sem = way * outer + b // inner
            return copy(ref, ref, self.send.at[sem], self.recv.at[q * n + b], (dev, f))

        def arrived(self, q, b):
            self.hop(q, b, 2).wait_recv()

        def own(self, q, way, act):
            def go():
                getattr(self.hop(q, s, way), act)()

            if way == 0:
                pl.when(z < outer - 1)(go)
            elif way == 1:
                pl.when(z > 0)(go)
            elif inner == 2:
                go()

        def mates(self, act):
            for q, (_, _, late) in enumerate(pieces):
                if late:
                    @pl.when(is_end(z))
                    def _(q=q):
                        if act == "start":
                            self.arrived(q, mate)
                        pl.when(z < outer - 1)(lambda: getattr(self.hop(q, mate, 0), act)())
                        pl.when(z > 0)(lambda: getattr(self.hop(q, mate, 1), act)())

        def relay(self, q, d, act):
            late = pieces[q][2]

            def one(b, way, to_mate):
                more = z < last if way == 0 else z > 0
                if self.deferred:
                    more = jnp.logical_and(more, jnp.logical_not(
                        jnp.logical_and(z == last - 1, b // inner == 0) if way == 0
                        else jnp.logical_and(z == 1, b // inner == last)))
                if act == "start":
                    self.arrived(q, b)
                pl.when(more)(lambda: getattr(self.hop(q, b, way), act)())
                if to_mate:
                    getattr(self.hop(q, b, 2), act)()

            def pass_on(level, way):
                if late:
                    end = is_end(level)

                    @pl.when(end)
                    def _():
                        for line in range(inner):
                            one(level * inner + line, way, False)

                    pl.when(jnp.logical_not(end))(lambda: one(level * inner + y, way, True))
                else:
                    one(level * inner + y, way, inner == 2)

            pl.when(z >= d)(lambda: pass_on(z - d, 0))
            pl.when(z + d < outer)(lambda: pass_on(z + d, 1))

        def held(self, way, act):
            def run():
                for q, (_, _, late) in enumerate(pieces):
                    for line in range(inner) if late else (y,):
                        level = last if way == 1 else 0
                        getattr(self.hop(q, level * inner + line, way), act)()

            pl.when(z == (1 if way == 1 else last - 1))(run)

        def finish(self, low=0, high=outer):
            if inner == 2:
                def step(level):
                    for q, (_, _, late) in enumerate(pieces):
                        def go(q=q):
                            self.arrived(q, level * inner + (1 - y))

                        if late:
                            pl.when(jnp.logical_not(is_end(level)))(go)
                        else:
                            go()

                loop(low, high, step)

    def move_weights(act):
        for gather in (wk_gather, wv_gather):
            for q in range(len(pieces)):
                gather.own(q, 0, act)
                gather.own(q, 1, act)
            for q in range(len(pieces) - 1, -1, -1):
                gather.own(q, 2, act)
            gather.mates(act)

    def relay_weights(act, low, high):
        def step(d):
            for gather in (wk_gather, wv_gather):
                for q in range(len(pieces)):
                    gather.relay(q, d, act)

        loop(low, high, step)

    def when_host(act):
        pl.when(jnp.logical_or(z == 1, z == last - 1))(act)

    class Guest:
        def __init__(self):
            self.span = inner * rows
            self.part = self.span // nf

        def place(self, p):
            return xg.at[:, pl.ds(pl.multiple_of(p * self.part, 128), self.part)]

        def move(self, p, sem, dev):
            return copy(self.place(p), self.place(p), xe_s.at[sem], xe_r.at[p], dev)

        def arrived(self, p):
            self.move(p, 0, (s, f)).wait_recv()

        def leave(self, act):
            @pl.when(is_end(z))
            def _():
                host = jnp.minimum(jnp.maximum(z, 1), last - 1) * inner + y
                at = pl.multiple_of((last - z) * self.span + f * self.part, 128)
                getattr(copy(x_ref.at[:, pl.ds(at, self.part)], self.place(f), xe_s.at[0],
                             xe_r.at[f], (host, f)), act)()

        def spread(self, act):
            def run():
                if act == "start":
                    self.arrived(f)
                loop(1, chips, lambda d: getattr(self.move(
                    f, d, (s, (chip + d) % chips * cores + core)), act)())
                if cores == 2:
                    getattr(self.move(f, chips + chip, (s, twin)), act)()

            when_host(run)

        def share(self, act):
            def step(d):
                o = (chip + d) % chips
                if act == "start":
                    self.arrived(o * cores + core)
                if cores == 2:
                    getattr(self.move(o * cores + core, chips + o, (s, twin)), act)()

            when_host(lambda: loop(1, chips, step))

        def finish(self):
            if cores == 2:
                loop(0, chips, lambda o: self.arrived(o * cores + 1 - core))

        def reply(self, i):
            end = jnp.minimum(z - 1, 1) * last
            return copy(pe_send.at[i], pe_recv.at[i], pe_s.at[i], pe_r.at[i], (end * inner + y, f))

        def partial(self, i, weights):
            def run():
                at = (last - jnp.minimum(z - 1, 1) * last) * self.span
                w = weights[pl.ds(pl.multiple_of(at, 16), self.span), :]
                pe_send[i] = dot_nn(xg[...], w).astype(BF16)
                self.reply(i).start()

            when_host(run)

        def rest(self, weights):
            at = pl.multiple_of(z // last * self.span, 128)
            here = pl.ds(at, (outer - 1) * self.span)
            return dot_nn(x_ref[:, here], weights[here, :])

        def returned(self, i):
            copy(pe_send.at[i], pe_recv.at[i], pe_s.at[i], pe_r.at[i], (mate, f)).wait_recv()
            return pe_recv[i].astype(F32)

        def drain(self):
            self.leave("wait_send")
            self.spread("wait_send")
            self.share("wait_send")
            when_host(lambda: loop(0, 2, lambda i: self.reply(i).wait_send()))

    wk_gather = Weights(wk_all, wk_s, wk_r)
    wv_gather = Weights(wv_all, wv_s, wv_r, deferred=hosted)
    guests = Guest() if hosted else None
    k_gather = Gather(k_all, k_s, k_r, causal=True)
    v_gather = Gather(v_all, v_s, v_r, causal=True)
    dk_gather = Gather(dk_all, *((v_s, v_r) if exchange else (dk_s, dk_r)))
    dv_gather = Gather(dv_all, *((k_s, k_r) if exchange else (dv_s, dv_r)))

    for load in loads[:3]:
        load.wait()
    if hosted:
        guests.leave("start")
    move_weights("start")
    for load in loads[3:]:
        load.wait()

    own_rows = pl.ds(pl.multiple_of(s * tok, tok), tok)
    if exchange:
        own_part = pl.ds(pl.multiple_of(f * part, 128), part)

        def x_src(b):
            return x_ref.at[:, pl.ds(pl.multiple_of(b * rows + f * part, 128), part)]

        def x_slot(b, at):
            return x_all.at[pl.ds(pl.multiple_of(b * tok, tok), tok), at]

        def x_copy(b):
            return copy(x_src(b), x_slot(s, own_part), x_s.at[b], x_r.at[s], (b, f))

        def x_arrived(b):
            copy(x_src(b), x_slot(b, own_part), x_s.at[b], x_r.at[b], (b, f)).wait_recv()

        def xf_copy(d):
            ref = x_all.at[:, own_part]
            return copy(ref, ref, xf_s.at[d], xf_r.at[f], (s, (f + d) % nf))

        def xf_arrived(d):
            b = (f + d) % nf
            ref = x_all.at[:, pl.ds(pl.multiple_of(b * part, 128), part)]
            copy(ref, ref, xf_s.at[d], xf_r.at[b], (s, b)).wait_recv()

        x_all[own_rows, own_part] = x_ref[
            :, pl.ds(pl.multiple_of(s * rows + f * part, 128), part)]

    for g in range(group):
        at = slice(g * tok, (g + 1) * tok)
        q_st[at, :] = q_ref[:, g * HD:(g + 1) * HD]
        up = g_ref[:, g * HD:(g + 1) * HD]
        g_st[at, :] = up
        g_tr[:, at] = up.astype(F32).T
    lane = lax.broadcasted_iota(jnp.int32, (tok, HD), 1)
    position = (s * tok + lax.broadcasted_iota(jnp.int32, (tok, HD), 0)).astype(F32)
    angle = position * freq_ref[...]
    cos_scr[...] = jnp.cos(angle)
    sin_scr[...] = jnp.where(lane < HD // 2, -jnp.sin(angle), jnp.sin(angle))

    def tell(which, device):
        pl.semaphore_signal(
            told.at[which], inc=1, device_id=(device, f), device_id_type=MESH)

    if hosted:
        pl.when(z < last - 1)(lambda: pl.semaphore_wait(told.at[0], 1))
        pl.when(jnp.logical_and(z > 0, z < last))(lambda: tell(0, s - inner))

        @pl.when(z == 0)
        def _():
            tell(1, mate)
            pl.semaphore_wait(told.at[1], 1)

    relay_weights("start", 1, 2)
    if hosted:
        guests.spread("start")
    relay_weights("start", 2, outer - 1)
    if hosted:
        guests.share("start")
    def x_ahead():
        loop(inner * (z + 1), n, lambda b: x_copy(b).start())

    if hosted:
        pl.when(z == 0)(x_ahead)

    def last_relays(act, gathers):
        for gather in gathers:
            for q in range(len(pieces)):
                gather.relay(q, outer - 1, act)

    def rotated(lin):
        return lin * cos_scr[...] + pltpu.roll(lin, HD // 2, 1) * sin_scr[...]

    def finish_levels(low, high):
        wk_gather.finish(low, high)
        wv_gather.finish(low, high)

    def keep_keys(lin):
        k_all[own_rows, :] = rotated(lin).astype(BF16)
        k_gather.start()

    def keep_values(value):
        v_all[own_rows, :] = value.astype(BF16)
        v_gather.start()

    def project():
        keep_keys(dot_nn(x_ref[...], wk_all[...]))
        keep_values(dot_nn(x_ref[...], wv_all[...]))

    def project_end():
        first = jnp.minimum(z, 1)
        with jax.named_scope("wkfin"):
            finish_levels(first, first + outer - 1)
        with jax.named_scope("kproj"):
            keys, values = guests.rest(wk_all), guests.rest(wv_all)
        with jax.named_scope("xfin"):
            keep_keys(keys + guests.returned(0))
        with jax.named_scope("vproj"):
            keep_values(values + guests.returned(1))

    def project_inner():
        with jax.named_scope("wkfin"):
            finish_levels(0, outer)
        with jax.named_scope("xfin"):
            pl.when(z < last - 1)(x_ahead)
            when_host(guests.finish)
        with jax.named_scope("kproj"):
            guests.partial(0, wk_all)
            guests.partial(1, wv_all)
        with jax.named_scope("vproj"):
            project()

    if hosted:
        pl.when(is_end(z))(project_end)
        pl.when(jnp.logical_not(is_end(z)))(project_inner)
    else:
        if outer > 1:
            last_relays("start", (wk_gather, wv_gather))
        finish_levels(0, outer)
        project()
    if hosted:
        wv_gather.held(1, "start")
    if exchange:
        pl.when(z == last - 1)(x_ahead) if hosted else x_ahead()
        loop(0, s, lambda b: x_copy(b).start())
    k_gather.forward()
    v_gather.forward()
    if hosted:
        last_relays("start", (wk_gather,))
    k_gather.finish()
    def each_span(step):
        if spans == 1:
            step(0)
        else:
            loop(0, s * tok // span + 1, lambda i: step(pl.multiple_of(i * span, span)))

    def at_chunk(base, c):
        return pl.ds(base + c * chunk, chunk)

    def fold(value):
        return value.reshape(chunk // 8, 8, m_cols)

    column = jnp.concatenate(
        [lax.broadcasted_iota(jnp.int32, (chunk, tok), 1)] * group, axis=1)
    ahead = lax.broadcasted_iota(jnp.int32, (chunk, m_cols), 0) - column

    m_scr[...] = jnp.full(m_scr.shape, NEG, F32)
    l_scr[...] = jnp.zeros(l_scr.shape, F32)
    o_acc[...] = jnp.zeros(o_acc.shape, F32)
    dq_acc[...] = jnp.zeros(dq_acc.shape, F32)

    def score(base):
        for c in range(span // chunk):
            sc = dot_nt(k_all[at_chunk(base, c), :], q_st[...])
            sc = jnp.where(ahead <= s * tok - base - c * chunk, sc, NEG)
            s_scr[at_chunk(base, c), :] = sc
            m_scr[...] = jnp.maximum(m_scr[...], jnp.max(fold(sc), axis=0))

    each_span(score)
    top = jnp.max(m_scr[...], axis=0, keepdims=True)

    def weigh(base):
        for c in range(span // chunk):
            e = jnp.exp2((s_scr[at_chunk(base, c), :] - top) * (scale * math.log2(math.e)))
            s_scr[at_chunk(base, c), :] = e
            l_scr[...] += jnp.sum(fold(e), axis=0)

    each_span(weigh)
    inverse = 1.0 / jnp.sum(l_scr[...], axis=0, keepdims=True)

    half = n // 2 if n % 2 == 0 else 0
    low_end = s // half * half if half else 0

    class Reduce:
        def __init__(self, send, recv, send_sem, recv_sem, own, sent):
            self.send, self.recv, self.send_sem, self.recv_sem = send, recv, send_sem, recv_sem
            self.own, self.sent = own, sent

        def direct(self, j):
            return copy(self.send.at[j], self.recv.at[s], self.send_sem.at[j], self.recv_sem.at[s],
                        (j, f))

        def inward(self, j):
            slot = n + s - half
            return copy(self.send.at[j], self.recv.at[slot], self.send_sem.at[j],
                        self.recv_sem.at[slot], (j + half, f))

        def got(self, slot):
            copy(self.send.at[0], self.recv.at[slot], self.send_sem.at[0], self.recv_sem.at[slot],
                 (mate, f)).wait_recv()
            return self.recv[slot].astype(F32)

        def hand(self, low, high, act):
            high = jnp.minimum(high, s)
            loop(jnp.maximum(low, low_end), high, lambda j: getattr(self.direct(j), act)())
            if half:
                @pl.when(s >= half)
                def _():
                    loop(low, jnp.minimum(high, half), lambda j: pl.when(j + half != s)(
                        lambda: getattr(self.inward(j), act)()))

        def pass_on(self):
            if half:
                @pl.when(s >= half)
                def _():
                    def add(i):
                        self.sent[...] += self.got(n + i - half)

                    loop(half, s, add)
                    loop(s + 1, n, add)
                    self.send[s - half] = self.sent[...].astype(BF16)
                    self.direct(s - half).start()

        def take(self):
            def add(j):
                self.own[...] += self.got(j)

            loop(s + 1, low_end + half if half else n, add)
            if half:
                pl.when(s < half)(lambda: add(s + half))

        def drain(self):
            self.hand(0, n, "wait_send")
            if half:
                pl.when(s >= half)(lambda: self.direct(s - half).wait_send())

    rk = Reduce(rk_send, rk_recv, rk_s, rk_r, own_dk, sent_dk)
    rv = Reduce(rv_send, rv_recv, rv_s, rv_r, own_dv, sent_dv)

    def hand_out(base, low, high, partial, reduce):
        first = base // tok
        reduce.hand(first + low, first + high, "start")

        def keep(block, out):
            at = pl.ds(pl.multiple_of((block - first) * tok, tok), tok)
            out[...] = partial[at, :]

        if spans == 1:
            if high == per_span:
                keep(s, reduce.own)
                if half:
                    pl.when(s >= half)(lambda: keep(s - half, reduce.sent))
        else:
            for block, out in ((s, reduce.own), (s - half, reduce.sent)):
                @pl.when(jnp.logical_and(block >= first + low, block < first + high))
                def _(block=block, out=out):
                    keep(block, out)

    def store_parts(base, c, value, partial, send):
        partial[c * chunk:(c + 1) * chunk, :] = value
        for i in range(chunk // tok):
            send[base // tok + c * (chunk // tok) + i] = value[i * tok:(i + 1) * tok].astype(BF16)

    def value_part(base):
        for c in range(span // chunk):
            p = s_scr[at_chunk(base, c), :] * inverse
            s_scr[at_chunk(base, c), :] = p
            low = p.astype(BF16)
            p_scr[at_chunk(base, c), :] = low
            store_parts(base, c, dot_nn(low, g_st[...]), dvp, rv_send)
        hand_out(base, 0, per_span, dvp, rv)

    each_span(value_part)
    v_gather.finish()
    if exchange:
        loop(s + 1, inner * (z + 1), lambda b: x_copy(b).start())

    def weighted(base):
        o_acc[...] += dot_tn(v_all[pl.ds(base, span), :], p_scr[pl.ds(base, span), :])

    each_span(weighted)
    delta = jnp.sum(g_tr[...] * o_acc[...], axis=0, keepdims=True)

    def key_part(base):
        halves = 2 if (span // chunk) % 2 == 0 else 1
        count = span // chunk // halves
        for part_of in range(halves):
            for c in range(part_of * count, (part_of + 1) * count):
                dp = dot_nt(v_all[at_chunk(base, c), :], g_st[...])
                ds = (s_scr[at_chunk(base, c), :] * (dp - delta)).astype(BF16)
                ds_scr[c * chunk:(c + 1) * chunk, :] = ds
                store_parts(base, c, dot_nn(ds, q_st[...]), dkp, rk_send)
            hand_out(base, part_of * per_span // halves, (part_of + 1) * per_span // halves, dkp, rk)
        dq_acc[...] += dot_tn(k_all[pl.ds(base, span), :], ds_scr[...])

    each_span(key_part)
    if hosted:
        wv_gather.held(0, "start")
    for g in range(group):
        at = slice(g * tok, (g + 1) * tok)
        ao_ref[:, g * HD:(g + 1) * HD] = o_acc[:, at].T.astype(BF16)
        gq_ref[:, g * HD:(g + 1) * HD] = (dq_acc[:, at] * scale).T.astype(BF16)


    if exchange:
        loop(0, s, x_arrived)
        loop(s + 1, n, x_arrived)
        loop(1, nf, lambda d: xf_copy(d).start())
    def drain_early():
        move_weights("wait_send")
        relay_weights("wait_send", 1, outer)
        if hosted:
            for way in (0, 1):
                wv_gather.held(way, "wait_send")
            guests.drain()
        if exchange:
            loop(0, s, lambda b: x_copy(b).wait_send())
            loop(s + 1, n, lambda b: x_copy(b).wait_send())

    for gather in (k_gather, v_gather):
        gather.drain()
    rv.pass_on()
    rk.pass_on()
    @pl.when(z < outer // 2)
    def _():
        if hosted:
            pl.when(z == 0)(lambda: last_relays("start", (wv_gather,)))
        drain_early()

    if hosted:
        pl.when(z > outer // 2)(lambda: pl.semaphore_wait(told.at[0], 1))

        @pl.when(jnp.logical_and(z >= outer // 2, z < last))
        def _():
            if cores == 2:
                pl.semaphore_signal(
                    told.at[1], inc=1, device_id=(s, twin), device_id_type=MESH)
                pl.semaphore_wait(told.at[1], 1)
            tell(0, s + inner)

    rv.take()
    dv_all[own_rows, :] = own_dv[...].astype(BF16)
    dv_gather.start()
    rk.take()
    lin = own_dk[...] * scale
    turned = lin * cos_scr[...] - pltpu.roll(lin, HD // 2, 1) * sin_scr[...]
    dk_all[own_rows, :] = turned.astype(BF16)
    dk_gather.start()

    def input_term(b):
        at = pl.ds(pl.multiple_of(b * width, width), width)
        return (dot_nt(dk_all[own_rows, :], wk_all[at, :])
                + dot_nt(dv_all[own_rows, :], wv_all[at, :]))

    def gi_twin(o):
        return copy(gi_send.at[o], gi_recv.at[o], gi_s.at[o], gi_r.at[o], (s, twin))

    def gi_far(d):
        return copy(gi_send.at[chips + d], gi_recv.at[chips + chip], gi_s.at[chips + d],
                    gi_r.at[chips + chip], (s, (chip + d) % chips * cores + core))

    def twin_term(d):
        o = (chip + d) % chips
        gi_send[o] = input_term(o * cores + 1 - core).astype(BF16)
        gi_twin(o).start()

    def own_term(d):
        o = (chip + d) % chips
        gi_own[o] = input_term(o * cores + core)

    def join(d):
        o = (chip + d) % chips
        gi_twin(o).wait_recv()
        gi_own[o] += gi_recv[o].astype(F32)

    def far_term(d):
        if cores == 2:
            join(d)
        gi_send[chips + d] = gi_own[(chip + d) % chips].astype(BF16)
        gi_far(d).start()

    def far_terms(d):
        if cores == 2:
            twin_term(d)
        own_term(d)
        far_term(d)

    if hosted:
        pl.when(z == last)(lambda: last_relays("start", (wv_gather,)))

        @pl.when(is_end(z))
        def _():
            for gather in (wk_gather, wv_gather):
                gather.finish(last - z, last - z + 1)

    loop(1, chips, far_terms)
    if cores == 2:
        twin_term(0)
    own_term(0)

    def weight_grad(grads, out):
        if exchange:
            out[...] = dot_tn(grads[...], x_all[...]).T
        else:
            grad = None
            step = min(total, 1024)
            for at in range(0, total, step):
                term = dot_tn(xt_in[at:at + step, :], grads[at:at + step, :])
                grad = term if grad is None else grad + term
            out[...] = grad

    pl.when(z >= outer // 2)(drain_early)
    dv_gather.forward()
    dk_gather.forward()
    dv_gather.finish()
    if exchange:
        loop(1, nf, xf_arrived)
    weight_grad(dv_all, gwv_ref)
    dk_gather.finish()
    weight_grad(dk_all, gwk_ref)

    def gi_take(d):
        b = (chip + d) % chips
        copy(gi_send.at[chips + d], gi_recv.at[chips + b], gi_s.at[chips + d],
             gi_r.at[chips + b], (s, b * cores + core)).wait_recv()
        gi_own[chip] += gi_recv[chips + b].astype(F32)

    if cores == 2:
        join(0)
    loop(1, chips, gi_take)
    gi_ref[...] = gi_own[chip].astype(BF16)

    for gather in (dk_gather, dv_gather):
        gather.drain()
    if exchange:
        loop(1, nf, lambda d: xf_copy(d).wait_send())
    rv.drain()
    rk.drain()
    if cores == 2:
        loop(0, chips, lambda o: gi_twin(o).wait_send())
    loop(1, chips, lambda d: gi_far(d).wait_send())


def publish(*refs):
    count = len(refs) // 2
    sems = refs[-1]
    moves = [pltpu.make_async_copy(refs[i], refs[count + i], sems.at[i]) for i in range(count)]
    for move in moves:
        move.start()
    for move in moves:
        move.wait()


def body(n, nf, queries, layer_input, w_key, w_value, grad_out):
    tok, depth = layer_input.shape
    rows, cols = w_key.shape
    assert cols == HD
    group = queries.shape[1] // cols
    m_cols = group * tok
    part = rows // nf
    exchange = part % 128 == 0
    half = HD // 2
    freq = np.float32(ROPE_BASE) ** (-(np.arange(half, dtype=np.float32) * np.float32(2.0 / HD)))
    freq = jnp.asarray(np.concatenate([freq, freq])[None, :], F32)
    operands = [queries, layer_input, w_key, w_value, grad_out, freq]
    if not exchange:
        operands.append(
            lax.all_to_all(layer_input, "seq", split_axis=1, concat_axis=0, tiled=True))
    width = depth // nf
    total = n * tok
    span = math.gcd(total, 1024)
    inner = 2 if n % 2 == 0 else 1
    outer = n // inner
    pieces = len(pieces_of(rows, inner))
    hops = 3 * outer + (2 * n + outer if pieces > 1 else 0)
    vmem = pltpu.VMEM
    dma = pltpu.SemaphoreType.DMA
    scratch = [vmem((depth, cols), BF16)] * 2
    scratch += [vmem((total, cols), BF16)] * 4
    scratch += [
        vmem((total, rows) if exchange else (16, 128), BF16),
        vmem((m_cols, HD), BF16), vmem((m_cols, HD), BF16), vmem((HD, m_cols), F32),
        vmem((total, m_cols), F32), vmem((total, m_cols), BF16), vmem((span, m_cols), BF16),
        vmem((8, m_cols), F32), vmem((8, m_cols), F32),
        vmem((HD, m_cols), F32), vmem((HD, m_cols), F32),
        vmem((span, cols), F32), vmem((span, cols), F32),
    ]
    slots = n + n // 2
    scratch += [vmem((n, tok, cols), BF16), vmem((slots, tok, cols), BF16)] * 2
    scratch += [vmem((tok, cols), F32)] * 6
    scratch += [
        vmem((2 * nf, tok, width), BF16), vmem((2 * nf, tok, width), BF16),
        vmem((nf, tok, width), F32),
    ]
    scratch += [vmem((tok, inner * rows), BF16)]
    scratch += [vmem((2, tok, cols), BF16)] * 2
    scratch += [pltpu.SemaphoreType.REGULAR((2,))]
    scratch += [dma((2 * nf,)), dma((nf,)), dma((2,)), dma((2,))]
    scratch += [dma((hops,)), dma((pieces * n,))] * 2
    scratch += [dma((2 * outer + 1,)), dma((n,))] * 2
    scratch += [dma((1,)), dma((1,))] * 2 if exchange else [dma((2 * outer + 1,)), dma((n,))] * 2
    scratch += [dma((n,)), dma((n,)), dma((nf,)), dma((nf,))]
    scratch += [dma((n,)), dma((slots,))] * 2
    scratch += [dma((2 * nf,)), dma((2 * nf,))]
    scratch += [vmem(queries.shape, BF16), vmem((tok, depth), BF16), vmem(queries.shape, BF16),
                dma((5,))]
    out_shape = [
        jax.ShapeDtypeStruct(queries.shape, BF16),
        jax.ShapeDtypeStruct(queries.shape, BF16),
        jax.ShapeDtypeStruct((tok, width), BF16),
        jax.ShapeDtypeStruct((rows, cols), F32),
        jax.ShapeDtypeStruct((rows, cols), F32),
    ]
    spec = pl.BlockSpec(memory_space=pltpu.VMEM)
    whole = pl.BlockSpec(memory_space=pl.ANY)
    results = pl.pallas_call(
        functools.partial(kernel, (n, nf, exchange)),
        out_shape=[pltpu.VMEM(o.shape, o.dtype) for o in out_shape],
        in_specs=[whole] * 5 + [spec] * (len(operands) - 5),
        out_specs=[spec] * len(out_shape),
        scratch_shapes=scratch,
        compiler_params=pltpu.CompilerParams(
            collective_id=0, has_side_effects=True, vmem_limit_bytes=60 * 1024 * 1024),
    )(*operands)
    return tuple(pl.pallas_call(
        publish,
        out_shape=out_shape,
        in_specs=[spec] * len(out_shape),
        out_specs=[whole] * len(out_shape),
        scratch_shapes=[dma((len(out_shape),))],
        compiler_params=pltpu.CompilerParams(vmem_limit_bytes=8 * 1024 * 1024),
    )(*results))


def solution(mesh):
    placed = (
        P("seq", "fsdp"),
        P("seq", None),
        P("seq", "fsdp"),
        P("seq", "fsdp"),
        P("seq", "fsdp"),
    )
    return jax.shard_map(
        functools.partial(body, mesh.shape["seq"], mesh.shape["fsdp"]),
        mesh=mesh,
        in_specs=placed,
        out_specs=(P("seq", "fsdp"),) * 5,
        check_vma=False,
    )
```

```python
import functools
import math

import jax
import jax.numpy as jnp
import numpy as np
from jax import lax
from jax.experimental import pallas as pl
from jax.experimental.pallas import tpu as pltpu
from jax.sharding import PartitionSpec as P

HD = 128
ROPE_BASE = 500000.0
NEG = -1e30
MESH = pl.DeviceIdType.MESH
F32 = jnp.float32
BF16 = jnp.bfloat16


def loop(low, high, step):
    def run(i, carry):
        step(i)
        return carry

    lax.fori_loop(low, high, run, 0)


def dot_nn(a, b):
    return lax.dot_general(a, b, (((1,), (0,)), ((), ())), preferred_element_type=F32)


def dot_nt(a, b):
    return lax.dot_general(a, b, (((1,), (1,)), ((), ())), preferred_element_type=F32)


def dot_tn(a, b):
    return lax.dot_general(a, b, (((0,), (0,)), ((), ())), preferred_element_type=F32)


def block_of(ref, b, size):
    return ref.at[pl.ds(pl.multiple_of(b * size, size), size)]


def pieces_of(rows, inner):
    late = rows * 5 // 8 // 16 * 16 if inner == 2 else 0
    return [(0, rows - late, False)] + ([(rows - late, late, True)] if late else [])


def kernel(cfg, *refs):
    n, nf, exchange = cfg
    q_hbm, x_hbm, wk_ref, wv_ref, g_hbm, freq_ref = refs[:6]
    refs = refs[6:]
    if not exchange:
        xt_in = refs[0]
        refs = refs[1:]
    ao_ref, gq_ref, gi_ref, gwk_ref, gwv_ref = refs[:5]
    (wk_all, wv_all, k_all, v_all, dk_all, dv_all, x_all, q_st, g_st, g_tr,
     s_scr, p_scr, ds_scr, m_scr, l_scr, o_acc, dq_acc, dkp, dvp,
     rk_send, rk_recv, rv_send, rv_recv, own_dk, own_dv, sent_dk, sent_dv, cos_scr, sin_scr,
     gi_send, gi_recv, gi_own, xg, pe_send, pe_recv,
     told, xe_s, xe_r, pe_s, pe_r, wk_s, wk_r, wv_s, wv_r, k_s, k_r, v_s, v_r, dk_s, dk_r, dv_s, dv_r,
     x_s, x_r, xf_s, xf_r, rk_s, rk_r, rv_s, rv_r, gi_s, gi_r,
     q_ref, x_ref, g_ref, in_s) = refs[5:]
    tok = x_ref.shape[0]
    rows, cols = wk_ref.shape
    group = q_ref.shape[1] // cols
    m_cols = group * tok
    part = rows // nf
    width = gi_ref.shape[1]
    total = n * tok
    span = ds_scr.shape[0]
    spans = total // span
    per_span = span // tok
    chunk = math.gcd(span, 256)
    scale = HD ** (-0.5)
    s = lax.axis_index("seq")
    f = lax.axis_index("fsdp")
    inner = 2 if n % 2 == 0 else 1
    outer = n // inner
    z = s // inner
    y = s % inner
    mate = z * inner + (inner - 1 - y)
    last = outer - 1
    hosted = exchange and inner == 2 and outer >= 4
    cores = 2 if nf % 2 == 0 else 1
    chips = nf // cores
    chip = f // cores
    core = f % cores
    twin = chip * cores + (cores - 1 - core)

    def copy(src, dst, send, recv, dev):
        return pltpu.make_async_remote_copy(
            src_ref=src, dst_ref=dst, send_sem=send, recv_sem=recv, device_id=dev,
            device_id_type=MESH,
        )

    barrier = pltpu.get_barrier_semaphore()

    def greet(b):
        pl.semaphore_signal(barrier, inc=1, device_id=(b, f), device_id_type=MESH)

    def greet_fsdp(d):
        pl.semaphore_signal(
            barrier, inc=1, device_id=(s, (f + d) % nf), device_id_type=MESH)

    pl.when(z < outer - 1)(lambda: greet(s + inner))
    pl.when(z > 0)(lambda: greet(s - inner))
    if inner == 2:
        greet(mate)
    loop(1, nf, greet_fsdp)
    loads = [
        pltpu.make_async_copy(src, dst, in_s.at[i])
        for i, (src, dst) in enumerate((
            (wk_ref, block_of(wk_all, s, rows)), (wv_ref, block_of(wv_all, s, rows)),
            (x_hbm, x_ref), (q_hbm, q_ref), (g_hbm, g_ref)))
    ]
    for load in loads:
        load.start()

    def clear(b):
        at = pl.ds(pl.multiple_of(b * tok, tok), tok)
        k_all[at, :] = jnp.zeros((tok, cols), BF16)
        v_all[at, :] = jnp.zeros((tok, cols), BF16)

    loop(inner * (z + 1), n, clear)
    pl.semaphore_wait(
        barrier, jnp.minimum(z, 1) + jnp.minimum(outer - 1 - z, 1) + nf + inner - 2)

    class Gather:
        def __init__(self, ref, send, recv, causal=False):
            self.slot = lambda b: block_of(ref, b, tok)
            self.send, self.recv, self.causal = send, recv, causal

        def move(self, b, sem, level, row):
            ref = self.slot(b)
            return copy(ref, ref, self.send.at[sem], self.recv.at[b], (level * inner + row, f))

        def arrived(self, b):
            self.move(b, 0, z, y).wait_recv()

        def ends(self):
            return z == 0 if self.causal else jnp.logical_or(z == 0, z == outer - 1)

        def sends(self, act):
            def run(sem, level, row):
                getattr(self.move(s, sem, level, row), act)()

            def near(d):
                pl.when(z + d < outer)(lambda: run(z + d, z + d, y))
                if not self.causal:
                    pl.when(z >= d)(lambda: run(z - d, z - d, y))

            def far():
                if inner == 2 and outer > 1:
                    pl.when(self.ends())(lambda: run(z, outer - 1 - z, 1 - y))

            def to_mate():
                if inner == 2:
                    run(outer, z, 1 - y)

            far()
            loop(0, outer - 1, lambda i: near(outer - 1 - i))
            to_mate()

        def start(self):
            self.sends("start")

        def relay(self, act, low=1, high=outer):
            def step(d):
                def pass_on(level):
                    b = level * inner + y
                    if act == "start":
                        self.arrived(b)
                    if inner == 2:
                        far = jnp.logical_or(level - z == outer - 1, z - level == outer - 1)
                        pl.when(jnp.logical_not(far))(lambda: getattr(
                            self.move(b, outer + 1 + level, z, 1 - y), act)())

                pl.when(z >= d)(lambda: pass_on(z - d))
                if not self.causal:
                    pl.when(z + d < outer)(lambda: pass_on(z + d))

            loop(low, high, step)

        def forward(self, low=1, high=outer):
            self.relay("start", low, high)

        def finish(self):
            if inner == 2:
                loop(0, z + 1 if self.causal else outer,
                     lambda level: self.arrived(level * inner + 1 - y))

        def drain(self):
            self.sends("wait_send")
            self.relay("wait_send")

    pieces = pieces_of(rows, inner)

    def is_end(level):
        return jnp.logical_or(level == 0, level == outer - 1)

    class Weights:
        def __init__(self, ref, send, recv, deferred=False):
            self.ref, self.send, self.recv, self.deferred = ref, send, recv, deferred

        def hop(self, q, b, way):
            at, count, late = pieces[q]
            ref = self.ref.at[pl.ds(pl.multiple_of(b * rows + at, 16), count)]
            dev = ((z + 1) * inner + y, (z - 1) * inner + y, mate)[way]
            if late:
                sem = 3 * outer + (2 * n + b // inner if way == 2 else way * n + b)
            else:
                sem = way * outer + b // inner
            return copy(ref, ref, self.send.at[sem], self.recv.at[q * n + b], (dev, f))

        def arrived(self, q, b):
            self.hop(q, b, 2).wait_recv()

        def own(self, q, way, act):
            def go():
                getattr(self.hop(q, s, way), act)()

            if way == 0:
                pl.when(z < outer - 1)(go)
            elif way == 1:
                pl.when(z > 0)(go)
            elif inner == 2:
                go()

        def mates(self, act):
            for q, (_, _, late) in enumerate(pieces):
                if late:
                    @pl.when(is_end(z))
                    def _(q=q):
                        if act == "start":
                            self.arrived(q, mate)
                        pl.when(z < outer - 1)(lambda: getattr(self.hop(q, mate, 0), act)())
                        pl.when(z > 0)(lambda: getattr(self.hop(q, mate, 1), act)())

        def relay(self, q, d, act):
            late = pieces[q][2]

            def one(b, way, to_mate):
                more = z < last if way == 0 else z > 0
                if self.deferred:
                    more = jnp.logical_and(more, jnp.logical_not(
                        jnp.logical_and(z == last - 1, b // inner == 0) if way == 0
                        else jnp.logical_and(z == 1, b // inner == last)))
                if act == "start":
                    self.arrived(q, b)
                pl.when(more)(lambda: getattr(self.hop(q, b, way), act)())
                if to_mate:
                    getattr(self.hop(q, b, 2), act)()

            def pass_on(level, way):
                if late:
                    end = is_end(level)

                    @pl.when(end)
                    def _():
                        for line in range(inner):
                            one(level * inner + line, way, False)

                    pl.when(jnp.logical_not(end))(lambda: one(level * inner + y, way, True))
                else:
                    one(level * inner + y, way, inner == 2)

            pl.when(z >= d)(lambda: pass_on(z - d, 0))
            pl.when(z + d < outer)(lambda: pass_on(z + d, 1))

        def held(self, way, act):
            def run():
                for q, (_, _, late) in enumerate(pieces):
                    for line in range(inner) if late else (y,):
                        level = last if way == 1 else 0
                        getattr(self.hop(q, level * inner + line, way), act)()

            pl.when(z == (1 if way == 1 else last - 1))(run)

        def finish(self, low=0, high=outer):
            if inner == 2:
                def step(level):
                    for q, (_, _, late) in enumerate(pieces):
                        def go(q=q):
                            self.arrived(q, level * inner + (1 - y))

                        if late:
                            pl.when(jnp.logical_not(is_end(level)))(go)
                        else:
                            go()

                loop(low, high, step)

    def move_weights(act):
        for gather in (wk_gather, wv_gather):
            for q in range(len(pieces)):
                gather.own(q, 0, act)
                gather.own(q, 1, act)
            for q in range(len(pieces) - 1, -1, -1):
                gather.own(q, 2, act)
            gather.mates(act)

    def relay_weights(act, low, high):
        def step(d):
            for gather in (wk_gather, wv_gather):
                for q in range(len(pieces)):
                    gather.relay(q, d, act)

        loop(low, high, step)

    def when_host(act):
        pl.when(jnp.logical_or(z == 1, z == last - 1))(act)

    class Guest:
        def __init__(self):
            self.span = inner * rows
            self.part = self.span // nf

        def place(self, p):
            return xg.at[:, pl.ds(pl.multiple_of(p * self.part, 128), self.part)]

        def move(self, p, sem, dev):
            return copy(self.place(p), self.place(p), xe_s.at[sem], xe_r.at[p], dev)

        def arrived(self, p):
            self.move(p, 0, (s, f)).wait_recv()

        def leave(self, act):
            @pl.when(is_end(z))
            def _():
                host = jnp.minimum(jnp.maximum(z, 1), last - 1) * inner + y
                at = pl.multiple_of((last - z) * self.span + f * self.part, 128)
                getattr(copy(x_ref.at[:, pl.ds(at, self.part)], self.place(f), xe_s.at[0],
                             xe_r.at[f], (host, f)), act)()

        def spread(self, act):
            def run():
                if act == "start":
                    self.arrived(f)
                loop(1, chips, lambda d: getattr(self.move(
                    f, d, (s, (chip + d) % chips * cores + core)), act)())
                if cores == 2:
                    getattr(self.move(f, chips + chip, (s, twin)), act)()

            when_host(run)

        def share(self, act):
            def step(d):
                o = (chip + d) % chips
                if act == "start":
                    self.arrived(o * cores + core)
                if cores == 2:
                    getattr(self.move(o * cores + core, chips + o, (s, twin)), act)()

            when_host(lambda: loop(1, chips, step))

        def finish(self):
            if cores == 2:
                loop(0, chips, lambda o: self.arrived(o * cores + 1 - core))

        def reply(self, i):
            end = jnp.minimum(z - 1, 1) * last
            return copy(pe_send.at[i], pe_recv.at[i], pe_s.at[i], pe_r.at[i], (end * inner + y, f))

        def partial(self, i, weights):
            def run():
                at = (last - jnp.minimum(z - 1, 1) * last) * self.span
                w = weights[pl.ds(pl.multiple_of(at, 16), self.span), :]
                pe_send[i] = dot_nn(xg[...], w).astype(BF16)
                self.reply(i).start()

            when_host(run)

        def rest(self, weights):
            at = pl.multiple_of(z // last * self.span, 128)
            here = pl.ds(at, (outer - 1) * self.span)
            return dot_nn(x_ref[:, here], weights[here, :])

        def returned(self, i):
            copy(pe_send.at[i], pe_recv.at[i], pe_s.at[i], pe_r.at[i], (mate, f)).wait_recv()
            return pe_recv[i].astype(F32)

        def drain(self):
            self.leave("wait_send")
            self.spread("wait_send")
            self.share("wait_send")
            when_host(lambda: loop(0, 2, lambda i: self.reply(i).wait_send()))

    wk_gather = Weights(wk_all, wk_s, wk_r)
    wv_gather = Weights(wv_all, wv_s, wv_r, deferred=hosted)
    guests = Guest() if hosted else None
    k_gather = Gather(k_all, k_s, k_r, causal=True)
    v_gather = Gather(v_all, v_s, v_r, causal=True)
    dk_gather = Gather(dk_all, *((v_s, v_r) if exchange else (dk_s, dk_r)))
    dv_gather = Gather(dv_all, *((k_s, k_r) if exchange else (dv_s, dv_r)))

    for load in loads[:3]:
        load.wait()
    if hosted:
        guests.leave("start")
    move_weights("start")
    for load in loads[3:]:
        load.wait()

    own_rows = pl.ds(pl.multiple_of(s * tok, tok), tok)
    if exchange:
        own_part = pl.ds(pl.multiple_of(f * part, 128), part)

        def x_src(b):
            return x_ref.at[:, pl.ds(pl.multiple_of(b * rows + f * part, 128), part)]

        def x_slot(b, at):
            return x_all.at[pl.ds(pl.multiple_of(b * tok, tok), tok), at]

        def x_copy(b):
            return copy(x_src(b), x_slot(s, own_part), x_s.at[b], x_r.at[s], (b, f))

        def x_arrived(b):
            copy(x_src(b), x_slot(b, own_part), x_s.at[b], x_r.at[b], (b, f)).wait_recv()

        def xf_copy(d):
            ref = x_all.at[:, own_part]
            return copy(ref, ref, xf_s.at[d], xf_r.at[f], (s, (f + d) % nf))

        def xf_arrived(d):
            b = (f + d) % nf
            ref = x_all.at[:, pl.ds(pl.multiple_of(b * part, 128), part)]
            copy(ref, ref, xf_s.at[d], xf_r.at[b], (s, b)).wait_recv()

        x_all[own_rows, own_part] = x_ref[
            :, pl.ds(pl.multiple_of(s * rows + f * part, 128), part)]

    for g in range(group):
        at = slice(g * tok, (g + 1) * tok)
        q_st[at, :] = q_ref[:, g * HD:(g + 1) * HD]
        up = g_ref[:, g * HD:(g + 1) * HD]
        g_st[at, :] = up
        g_tr[:, at] = up.astype(F32).T
    lane = lax.broadcasted_iota(jnp.int32, (tok, HD), 1)
    position = (s * tok + lax.broadcasted_iota(jnp.int32, (tok, HD), 0)).astype(F32)
    angle = position * freq_ref[...]
    cos_scr[...] = jnp.cos(angle)
    sin_scr[...] = jnp.where(lane < HD // 2, -jnp.sin(angle), jnp.sin(angle))

    def tell(which, device):
        pl.semaphore_signal(
            told.at[which], inc=1, device_id=(device, f), device_id_type=MESH)

    if hosted:
        pl.when(z < last - 1)(lambda: pl.semaphore_wait(told.at[0], 1))
        pl.when(jnp.logical_and(z > 0, z < last))(lambda: tell(0, s - inner))

        @pl.when(z == 0)
        def _():
            tell(1, mate)
            pl.semaphore_wait(told.at[1], 1)

    relay_weights("start", 1, 2)
    if hosted:
        guests.spread("start")
    relay_weights("start", 2, outer - 1)
    if hosted:
        guests.share("start")
    def x_ahead():
        loop(inner * (z + 1), n, lambda b: x_copy(b).start())

    if hosted:
        pl.when(z == 0)(x_ahead)

    def last_relays(act, gathers):
        for gather in gathers:
            for q in range(len(pieces)):
                gather.relay(q, outer - 1, act)

    def rotated(lin):
        return lin * cos_scr[...] + pltpu.roll(lin, HD // 2, 1) * sin_scr[...]

    def finish_levels(low, high):
        wk_gather.finish(low, high)
        wv_gather.finish(low, high)

    def keep_keys(lin):
        k_all[own_rows, :] = rotated(lin).astype(BF16)
        k_gather.start()

    def keep_values(value):
        v_all[own_rows, :] = value.astype(BF16)
        v_gather.start()

    def project():
        keep_keys(dot_nn(x_ref[...], wk_all[...]))
        keep_values(dot_nn(x_ref[...], wv_all[...]))

    def project_end():
        first = jnp.minimum(z, 1)
        with jax.named_scope("wkfin"):
            finish_levels(first, first + outer - 1)
        with jax.named_scope("kproj"):
            keys, values = guests.rest(wk_all), guests.rest(wv_all)
        with jax.named_scope("xfin"):
            keep_keys(keys + guests.returned(0))
        with jax.named_scope("vproj"):
            keep_values(values + guests.returned(1))

    def project_inner():
        with jax.named_scope("wkfin"):
            finish_levels(0, outer)
        with jax.named_scope("xfin"):
            pl.when(z < last - 1)(x_ahead)
            when_host(guests.finish)
        with jax.named_scope("kproj"):
            guests.partial(0, wk_all)
            guests.partial(1, wv_all)
        with jax.named_scope("vproj"):
            project()

    if hosted:
        pl.when(is_end(z))(project_end)
        pl.when(jnp.logical_not(is_end(z)))(project_inner)
    else:
        if outer > 1:
            last_relays("start", (wk_gather, wv_gather))
        finish_levels(0, outer)
        project()
    if hosted:
        wv_gather.held(1, "start")
    if exchange:
        pl.when(z == last - 1)(x_ahead) if hosted else x_ahead()
        loop(0, s, lambda b: x_copy(b).start())
    k_gather.forward()
    v_gather.forward()
    if hosted:
        last_relays("start", (wk_gather,))
    k_gather.finish()
    def each_span(step):
        if spans == 1:
            step(0)
        else:
            loop(0, s * tok // span + 1, lambda i: step(pl.multiple_of(i * span, span)))

    def at_chunk(base, c):
        return pl.ds(base + c * chunk, chunk)

    def fold(value):
        return value.reshape(chunk // 8, 8, m_cols)

    column = jnp.concatenate(
        [lax.broadcasted_iota(jnp.int32, (chunk, tok), 1)] * group, axis=1)
    ahead = lax.broadcasted_iota(jnp.int32, (chunk, m_cols), 0) - column

    m_scr[...] = jnp.full(m_scr.shape, NEG, F32)
    l_scr[...] = jnp.zeros(l_scr.shape, F32)
    o_acc[...] = jnp.zeros(o_acc.shape, F32)
    dq_acc[...] = jnp.zeros(dq_acc.shape, F32)

    def score(base):
        for c in range(span // chunk):
            sc = dot_nt(k_all[at_chunk(base, c), :], q_st[...])
            sc = jnp.where(ahead <= s * tok - base - c * chunk, sc, NEG)
            s_scr[at_chunk(base, c), :] = sc
            m_scr[...] = jnp.maximum(m_scr[...], jnp.max(fold(sc), axis=0))

    each_span(score)
    top = jnp.max(m_scr[...], axis=0, keepdims=True)

    def weigh(base):
        for c in range(span // chunk):
            e = jnp.exp2((s_scr[at_chunk(base, c), :] - top) * (scale * math.log2(math.e)))
            s_scr[at_chunk(base, c), :] = e
            l_scr[...] += jnp.sum(fold(e), axis=0)

    each_span(weigh)
    inverse = 1.0 / jnp.sum(l_scr[...], axis=0, keepdims=True)

    half = n // 2 if n % 2 == 0 else 0
    low_end = s // half * half if half else 0

    class Reduce:
        def __init__(self, send, recv, send_sem, recv_sem, own, sent):
            self.send, self.recv, self.send_sem, self.recv_sem = send, recv, send_sem, recv_sem
            self.own, self.sent = own, sent

        def direct(self, j):
            return copy(self.send.at[j], self.recv.at[s], self.send_sem.at[j], self.recv_sem.at[s],
                        (j, f))

        def inward(self, j):
            slot = n + s - half
            return copy(self.send.at[j], self.recv.at[slot], self.send_sem.at[j],
                        self.recv_sem.at[slot], (j + half, f))

        def got(self, slot):
            copy(self.send.at[0], self.recv.at[slot], self.send_sem.at[0], self.recv_sem.at[slot],
                 (mate, f)).wait_recv()
            return self.recv[slot].astype(F32)

        def hand(self, low, high, act):
            high = jnp.minimum(high, s)
            loop(jnp.maximum(low, low_end), high, lambda j: getattr(self.direct(j), act)())
            if half:
                @pl.when(s >= half)
                def _():
                    loop(low, jnp.minimum(high, half), lambda j: pl.when(j + half != s)(
                        lambda: getattr(self.inward(j), act)()))

        def pass_on(self):
            if half:
                @pl.when(s >= half)
                def _():
                    def add(i):
                        self.sent[...] += self.got(n + i - half)

                    loop(half, s, add)
                    loop(s + 1, n, add)
                    self.send[s - half] = self.sent[...].astype(BF16)
                    self.direct(s - half).start()

        def take(self):
            def add(j):
                self.own[...] += self.got(j)

            loop(s + 1, low_end + half if half else n, add)
            if half:
                pl.when(s < half)(lambda: add(s + half))

        def drain(self):
            self.hand(0, n, "wait_send")
            if half:
                pl.when(s >= half)(lambda: self.direct(s - half).wait_send())

    rk = Reduce(rk_send, rk_recv, rk_s, rk_r, own_dk, sent_dk)
    rv = Reduce(rv_send, rv_recv, rv_s, rv_r, own_dv, sent_dv)

    def hand_out(base, low, high, partial, reduce):
        first = base // tok
        reduce.hand(first + low, first + high, "start")

        def keep(block, out):
            at = pl.ds(pl.multiple_of((block - first) * tok, tok), tok)
            out[...] = partial[at, :]

        if spans == 1:
            if high == per_span:
                keep(s, reduce.own)
                if half:
                    pl.when(s >= half)(lambda: keep(s - half, reduce.sent))
        else:
            for block, out in ((s, reduce.own), (s - half, reduce.sent)):
                @pl.when(jnp.logical_and(block >= first + low, block < first + high))
                def _(block=block, out=out):
                    keep(block, out)

    def store_parts(base, c, value, partial, send):
        partial[c * chunk:(c + 1) * chunk, :] = value
        for i in range(chunk // tok):
            send[base // tok + c * (chunk // tok) + i] = value[i * tok:(i + 1) * tok].astype(BF16)

    def value_part(base):
        for c in range(span // chunk):
            p = s_scr[at_chunk(base, c), :] * inverse
            s_scr[at_chunk(base, c), :] = p
            low = p.astype(BF16)
            p_scr[at_chunk(base, c), :] = low
            store_parts(base, c, dot_nn(low, g_st[...]), dvp, rv_send)
        hand_out(base, 0, per_span, dvp, rv)

    each_span(value_part)
    v_gather.finish()
    if exchange:
        loop(s + 1, inner * (z + 1), lambda b: x_copy(b).start())

    def weighted(base):
        o_acc[...] += dot_tn(v_all[pl.ds(base, span), :], p_scr[pl.ds(base, span), :])

    each_span(weighted)
    delta = jnp.sum(g_tr[...] * o_acc[...], axis=0, keepdims=True)

    def key_part(base):
        halves = 2 if (span // chunk) % 2 == 0 else 1
        count = span // chunk // halves
        for part_of in range(halves):
            for c in range(part_of * count, (part_of + 1) * count):
                dp = dot_nt(v_all[at_chunk(base, c), :], g_st[...])
                ds = (s_scr[at_chunk(base, c), :] * (dp - delta)).astype(BF16)
                ds_scr[c * chunk:(c + 1) * chunk, :] = ds
                store_parts(base, c, dot_nn(ds, q_st[...]), dkp, rk_send)
            hand_out(base, part_of * per_span // halves, (part_of + 1) * per_span // halves, dkp, rk)
        dq_acc[...] += dot_tn(k_all[pl.ds(base, span), :], ds_scr[...])

    each_span(key_part)
    if hosted:
        wv_gather.held(0, "start")
    for g in range(group):
        at = slice(g * tok, (g + 1) * tok)
        ao_ref[:, g * HD:(g + 1) * HD] = o_acc[:, at].T.astype(BF16)
        gq_ref[:, g * HD:(g + 1) * HD] = (dq_acc[:, at] * scale).T.astype(BF16)


    if exchange:
        loop(0, s, x_arrived)
        loop(s + 1, n, x_arrived)
        loop(1, nf, lambda d: xf_copy(d).start())
    def drain_early():
        move_weights("wait_send")
        relay_weights("wait_send", 1, outer)
        if hosted:
            for way in (0, 1):
                wv_gather.held(way, "wait_send")
            guests.drain()
        if exchange:
            loop(0, s, lambda b: x_copy(b).wait_send())
            loop(s + 1, n, lambda b: x_copy(b).wait_send())

    for gather in (k_gather, v_gather):
        gather.drain()
    rv.pass_on()
    rk.pass_on()
    @pl.when(z < outer // 2)
    def _():
        if hosted:
            pl.when(z == 0)(lambda: last_relays("start", (wv_gather,)))
        drain_early()

    if hosted:
        pl.when(z > outer // 2)(lambda: pl.semaphore_wait(told.at[0], 1))

        @pl.when(jnp.logical_and(z >= outer // 2, z < last))
        def _():
            if cores == 2:
                pl.semaphore_signal(
                    told.at[1], inc=1, device_id=(s, twin), device_id_type=MESH)
                pl.semaphore_wait(told.at[1], 1)
            tell(0, s + inner)

    rv.take()
    dv_all[own_rows, :] = own_dv[...].astype(BF16)
    dv_gather.start()
    rk.take()
    lin = own_dk[...] * scale
    turned = lin * cos_scr[...] - pltpu.roll(lin, HD // 2, 1) * sin_scr[...]
    dk_all[own_rows, :] = turned.astype(BF16)
    dk_gather.start()

    def input_term(b):
        at = pl.ds(pl.multiple_of(b * width, width), width)
        return (dot_nt(dk_all[own_rows, :], wk_all[at, :])
                + dot_nt(dv_all[own_rows, :], wv_all[at, :]))

    def gi_twin(o):
        return copy(gi_send.at[o], gi_recv.at[o], gi_s.at[o], gi_r.at[o], (s, twin))

    def gi_far(d):
        return copy(gi_send.at[chips + d], gi_recv.at[chips + chip], gi_s.at[chips + d],
                    gi_r.at[chips + chip], (s, (chip + d) % chips * cores + core))

    def twin_term(d):
        o = (chip + d) % chips
        gi_send[o] = input_term(o * cores + 1 - core).astype(BF16)
        gi_twin(o).start()

    def own_term(d):
        o = (chip + d) % chips
        gi_own[o] = input_term(o * cores + core)

    def join(d):
        o = (chip + d) % chips
        gi_twin(o).wait_recv()
        gi_own[o] += gi_recv[o].astype(F32)

    def far_term(d):
        if cores == 2:
            join(d)
        gi_send[chips + d] = gi_own[(chip + d) % chips].astype(BF16)
        gi_far(d).start()

    def far_terms(d):
        if cores == 2:
            twin_term(d)
        own_term(d)
        far_term(d)

    if hosted:
        pl.when(z == last)(lambda: last_relays("start", (wv_gather,)))

        @pl.when(is_end(z))
        def _():
            for gather in (wk_gather, wv_gather):
                gather.finish(last - z, last - z + 1)

    loop(1, chips, far_terms)
    if cores == 2:
        twin_term(0)
    own_term(0)

    def weight_grad(grads, out):
        if exchange:
            out[...] = dot_tn(grads[...], x_all[...]).T
        else:
            grad = None
            step = min(total, 1024)
            for at in range(0, total, step):
                term = dot_tn(xt_in[at:at + step, :], grads[at:at + step, :])
                grad = term if grad is None else grad + term
            out[...] = grad

    dv_gather.forward()
    dk_gather.forward()
    pl.when(z >= outer // 2)(drain_early)
    dv_gather.finish()
    if exchange:
        loop(1, nf, xf_arrived)
    weight_grad(dv_all, gwv_ref)
    dk_gather.finish()
    weight_grad(dk_all, gwk_ref)

    def gi_take(d):
        b = (chip + d) % chips
        copy(gi_send.at[chips + d], gi_recv.at[chips + b], gi_s.at[chips + d],
             gi_r.at[chips + b], (s, b * cores + core)).wait_recv()
        gi_own[chip] += gi_recv[chips + b].astype(F32)

    if cores == 2:
        join(0)
    loop(1, chips, gi_take)
    gi_ref[...] = gi_own[chip].astype(BF16)

    for gather in (dk_gather, dv_gather):
        gather.drain()
    if exchange:
        loop(1, nf, lambda d: xf_copy(d).wait_send())
    rv.drain()
    rk.drain()
    if cores == 2:
        loop(0, chips, lambda o: gi_twin(o).wait_send())
    loop(1, chips, lambda d: gi_far(d).wait_send())


def publish(*refs):
    count = len(refs) // 2
    sems = refs[-1]
    moves = [pltpu.make_async_copy(refs[i], refs[count + i], sems.at[i]) for i in range(count)]
    for move in moves:
        move.start()
    for move in moves:
        move.wait()


def body(n, nf, queries, layer_input, w_key, w_value, grad_out):
    tok, depth = layer_input.shape
    rows, cols = w_key.shape
    assert cols == HD
    group = queries.shape[1] // cols
    m_cols = group * tok
    part = rows // nf
    exchange = part % 128 == 0
    half = HD // 2
    freq = np.float32(ROPE_BASE) ** (-(np.arange(half, dtype=np.float32) * np.float32(2.0 / HD)))
    freq = jnp.asarray(np.concatenate([freq, freq])[None, :], F32)
    operands = [queries, layer_input, w_key, w_value, grad_out, freq]
    if not exchange:
        operands.append(
            lax.all_to_all(layer_input, "seq", split_axis=1, concat_axis=0, tiled=True))
    width = depth // nf
    total = n * tok
    span = math.gcd(total, 1024)
    inner = 2 if n % 2 == 0 else 1
    outer = n // inner
    pieces = len(pieces_of(rows, inner))
    hops = 3 * outer + (2 * n + outer if pieces > 1 else 0)
    vmem = pltpu.VMEM
    dma = pltpu.SemaphoreType.DMA
    scratch = [vmem((depth, cols), BF16)] * 2
    scratch += [vmem((total, cols), BF16)] * 4
    scratch += [
        vmem((total, rows) if exchange else (16, 128), BF16),
        vmem((m_cols, HD), BF16), vmem((m_cols, HD), BF16), vmem((HD, m_cols), F32),
        vmem((total, m_cols), F32), vmem((total, m_cols), BF16), vmem((span, m_cols), BF16),
        vmem((8, m_cols), F32), vmem((8, m_cols), F32),
        vmem((HD, m_cols), F32), vmem((HD, m_cols), F32),
        vmem((span, cols), F32), vmem((span, cols), F32),
    ]
    slots = n + n // 2
    scratch += [vmem((n, tok, cols), BF16), vmem((slots, tok, cols), BF16)] * 2
    scratch += [vmem((tok, cols), F32)] * 6
    scratch += [
        vmem((2 * nf, tok, width), BF16), vmem((2 * nf, tok, width), BF16),
        vmem((nf, tok, width), F32),
    ]
    scratch += [vmem((tok, inner * rows), BF16)]
    scratch += [vmem((2, tok, cols), BF16)] * 2
    scratch += [pltpu.SemaphoreType.REGULAR((2,))]
    scratch += [dma((2 * nf,)), dma((nf,)), dma((2,)), dma((2,))]
    scratch += [dma((hops,)), dma((pieces * n,))] * 2
    scratch += [dma((2 * outer + 1,)), dma((n,))] * 2
    scratch += [dma((1,)), dma((1,))] * 2 if exchange else [dma((2 * outer + 1,)), dma((n,))] * 2
    scratch += [dma((n,)), dma((n,)), dma((nf,)), dma((nf,))]
    scratch += [dma((n,)), dma((slots,))] * 2
    scratch += [dma((2 * nf,)), dma((2 * nf,))]
    scratch += [vmem(queries.shape, BF16), vmem((tok, depth), BF16), vmem(queries.shape, BF16),
                dma((5,))]
    out_shape = [
        jax.ShapeDtypeStruct(queries.shape, BF16),
        jax.ShapeDtypeStruct(queries.shape, BF16),
        jax.ShapeDtypeStruct((tok, width), BF16),
        jax.ShapeDtypeStruct((rows, cols), F32),
        jax.ShapeDtypeStruct((rows, cols), F32),
    ]
    spec = pl.BlockSpec(memory_space=pltpu.VMEM)
    whole = pl.BlockSpec(memory_space=pl.ANY)
    results = pl.pallas_call(
        functools.partial(kernel, (n, nf, exchange)),
        out_shape=[pltpu.VMEM(o.shape, o.dtype) for o in out_shape],
        in_specs=[whole] * 5 + [spec] * (len(operands) - 5),
        out_specs=[spec] * len(out_shape),
        scratch_shapes=scratch,
        compiler_params=pltpu.CompilerParams(
            collective_id=0, has_side_effects=True, vmem_limit_bytes=60 * 1024 * 1024),
    )(*operands)
    return tuple(pl.pallas_call(
        publish,
        out_shape=out_shape,
        in_specs=[spec] * len(out_shape),
        out_specs=[whole] * len(out_shape),
        scratch_shapes=[dma((len(out_shape),))],
        compiler_params=pltpu.CompilerParams(vmem_limit_bytes=8 * 1024 * 1024),
    )(*results))


def solution(mesh):
    placed = (
        P("seq", "fsdp"),
        P("seq", None),
        P("seq", "fsdp"),
        P("seq", "fsdp"),
        P("seq", "fsdp"),
    )
    return jax.shard_map(
        functools.partial(body, mesh.shape["seq"], mesh.shape["fsdp"]),
        mesh=mesh,
        in_specs=placed,
        out_specs=(P("seq", "fsdp"),) * 5,
        check_vma=False,
    )
```
